128 devices in a mesh: run: 16 (over z, y_hi, core), strip: 8 (over y_lo, x).
Axes of the slice: x: 4, y: 4 (y_hi: 2, y_lo: 2; y = y_hi * 2 + y_lo), z: 4, core: 2. Of those that a mesh axis runs over, the one named last changes fastest.
Arguments:
- base_field: float32 [512, 8, 256], P('strip'), may hold values from -3 to 3
- material_map: int32 [512, 8, 256], P('strip'), may hold values from 0 to 3
- param_levels: float32 [6, 8], replicated, may hold values from 0.2 to 1
- param_index: int32 [64, 6], replicated, may hold values from 0 to 7
- w_input: float32 [8, 512], replicated, may hold values from -2 to 2
- w_output: bfloat16 [512, 512, 2048], P(None, 'strip', 'run'), may hold values from -0.375 to 0.375
Outputs:
- grad_output: bfloat16 [512, 512, 2048], P(None, 'strip', 'run')
- grad_input: float32 [8, 512], P(None, ('run', 'strip'))
The draws below stay inside these ranges and needn't reach their ends.
All inputs are finite; a program needn't handle non-finite values.
Results may differ from the reference program's by a relative error of at most 0.0025.
Values may be sent and summed in bfloat16 or wider, within the bound.
A program may use at most 128 MiB of HBM per device.

```python
import jax
import jax.numpy as jnp
from jax import lax

NX = 512
NZ = 8
NY = 256
HID = 512
NPARAM = 6
LEVELS = 8
STEPS = 4
RUNS = 64
BATCH = 256
NIN = 8
N_STRIP = 8


def with_ends(result, stream_key, low, largest):
    shape = result.shape
    index_at = [jax.random.randint(jax.random.fold_in(stream_key, axis), (), 0, shape[axis]) for axis in range(len(shape))]
    result = result.at[tuple(index_at)].set(low)
    longest = shape.index(max(shape))
    index_at[longest] = (index_at[longest] + 1) % shape[longest]
    return result.at[tuple(index_at)].set(largest)


def spiked(drawn, own_key, source, target, blocks, factor):
    def block_of(dim):
        return (jnp.arange(drawn.shape[dim]) // (drawn.shape[dim] // blocks)).reshape((-1,) + (1,) * (drawn.ndim - 1 - dim))

    first = jax.random.permutation(own_key, blocks)[block_of(target)]
    far = (block_of(target) + blocks // 2) % blocks
    return jnp.where((block_of(source) == first) | (block_of(source) == far), factor * drawn, drawn)


def block_scale(rng, dims, pieces, smallest, high):
    factor_of = 1.0
    for dim, parts in pieces:
        heights = jax.random.uniform(jax.random.fold_in(jax.random.fold_in(rng, 6), dim), (parts,), jnp.float32, smallest / len(pieces), high / len(pieces))
        factor_of = factor_of * jnp.repeat(jnp.exp(heights), dims[dim] // parts).reshape((-1,) + (1,) * (len(dims) - 1 - dim))
    return factor_of


def noise(stream_key, extent, deviation, most, pieces=(), kind=jnp.bfloat16):
    gain = block_scale(stream_key, extent, pieces, -0.22, 0.18) if pieces else 1.0
    drawn = jax.random.normal(stream_key, extent, jnp.float32) * deviation * gain
    return jnp.minimum(jnp.maximum(drawn, -most), most).astype(kind)


def gaussian_with(stream_key, extent, deviation, bound, cuts, heavy, kind=jnp.bfloat16):
    entries = deviation * jax.random.normal(stream_key, extent, jnp.float32)
    if cuts:
        entries = entries * block_scale(stream_key, extent, cuts, -0.22, 0.18)
    return jnp.clip(spiked(entries, jax.random.fold_in(stream_key, 3), *heavy), -bound, bound).astype(kind)


def setup_inputs(seed: int = 0) -> dict:
    key_list = jax.random.split(jax.random.key(seed), 7)
    base_field = noise(key_list[0], (NX, NZ, NY), 0.5, 3.0, ((0, 8),), jnp.float32)
    material_map = with_ends(jax.random.randint(key_list[1], (NX, NZ, NY), 0, 4), jax.random.fold_in(key_list[1], 1), 0, 3).astype(jnp.int32)
    param_levels = jnp.clip(jax.random.uniform(key_list[2], (NPARAM, LEVELS), jnp.float32, 0.2, 1.0), 0.2, 1.0)
    param_index = with_ends(jax.random.randint(key_list[3], (RUNS, NPARAM), 0, LEVELS), jax.random.fold_in(key_list[3], 1), 0, LEVELS - 1).astype(jnp.int32)
    w_input = noise(key_list[4], (NIN, HID), NIN ** -0.5, 2.0, (), jnp.float32)
    w_output = gaussian_with(key_list[5], (HID, NX, NZ * NY), HID ** -0.5, 0.375, ((1, 8), (2, 16)), (1, 0, 8, 2.0))
    return dict(base_field=base_field, material_map=material_map, param_levels=param_levels, param_index=param_index, w_input=w_input, w_output=w_output)


time_step = 0.08


def advance(upad, kpad):
    lead = (slice(None),) * (upad.ndim - 3)
    middle = (slice(1, -1), slice(1, -1), slice(1, -1))
    near = [
        (slice(2, None), slice(1, -1), slice(1, -1)),
        (slice(0, -2), slice(1, -1), slice(1, -1)),
        (slice(1, -1), slice(2, None), slice(1, -1)),
        (slice(1, -1), slice(0, -2), slice(1, -1)),
        (slice(1, -1), slice(1, -1), slice(2, None)),
        (slice(1, -1), slice(1, -1), slice(0, -2)),
    ]
    field = upad[lead + middle]
    conduct = kpad[lead + middle]
    flux = jnp.zeros_like(field)
    for place in near:
        other = upad[lead + place]
        other_k = kpad[lead + place]
        flux = flux + 0.5 * (conduct + other_k) * (other - field)
    return field + time_step * flux


def run_values(param_levels, param_index):
    levels = jnp.arange(param_levels.shape[1], dtype=jnp.int32)
    picks = (param_index[:, :, None] == levels[None, None, :]).astype(jnp.float32)
    return jnp.sum(picks * param_levels[None, :, :].astype(jnp.float32), axis=-1)


def cond_field(material_map, mine):
    cond = jnp.zeros(material_map.shape, jnp.float32) + mine[0]
    for mat in range(1, 4):
        cond = jnp.where(material_map == mat, mine[mat], cond)
    return cond


def make_features(values):
    count = values.shape[0]
    times = (jnp.arange(STEPS, dtype=jnp.float32) + 1.0) / STEPS
    left = jnp.broadcast_to(values[None], (STEPS, count, values.shape[1]))
    middle = jnp.broadcast_to(times[:, None, None], (STEPS, count, 1))
    right = jnp.ones((STEPS, count, 1), jnp.float32)
    return jnp.concatenate([left, middle, right], axis=-1).reshape(STEPS * count, values.shape[1] + 2)


def reference(base_field, material_map, param_levels, param_index, w_input, w_output):
    values = run_values(param_levels, param_index)

    def one_run(mine):
        cond = cond_field(material_map, mine)
        gamma = 0.1 * mine[4]
        field = mine[5] * base_field
        shots = []
        for step in range(STEPS):
            conduct = cond * (1.0 + gamma * field * field)
            field = advance(jnp.pad(field, 1), jnp.pad(conduct, 1))
            shots.append(field.astype(jnp.bfloat16))
        return jnp.stack(shots)

    snaps = lax.map(one_run, values)
    zy = NZ * NY
    xl = NX // N_STRIP
    target = jnp.transpose(snaps, (1, 0, 2, 3, 4)).reshape(BATCH, N_STRIP, xl * zy)
    target = jnp.transpose(target, (1, 0, 2))
    wblocks = jnp.transpose(w_output.reshape(HID, N_STRIP, xl * zy), (1, 0, 2))
    features = make_features(values)
    hidden = jnp.tanh(jnp.dot(features, w_input.astype(jnp.float32), precision=lax.Precision.HIGHEST))
    hidden_b = hidden.astype(jnp.bfloat16)
    scale = BATCH ** -0.5

    def block(back, pair):
        goal, weight = pair
        pred = jnp.dot(hidden_b, weight, preferred_element_type=jnp.float32)
        error = ((pred - goal.astype(jnp.float32)) * scale).astype(jnp.bfloat16)
        grad = lax.dot_general(hidden_b, error, (((0,), (0,)), ((), ())), preferred_element_type=jnp.float32)
        part = lax.dot_general(error, weight, (((1,), (1,)), ((), ())), preferred_element_type=jnp.float32)
        return back + part, grad.astype(jnp.bfloat16)

    back, grads = lax.scan(block, jnp.zeros((BATCH, HID), jnp.float32), (target, wblocks))
    grad_output = jnp.transpose(grads.reshape(N_STRIP, HID, xl, zy), (1, 0, 2, 3)).reshape(HID, NX, zy)
    slope = back * (1.0 - hidden * hidden)
    grad_input = jnp.dot(features.T, slope, precision=lax.Precision.HIGHEST)
    return grad_output, grad_input
```

```python
import functools

import jax
import jax.numpy as jnp
from jax import lax
from jax.experimental import pallas as pl
from jax.experimental.pallas import tpu as pltpu
from jax.sharding import PartitionSpec as P

STEPS = 4
TIME_STEP = 0.08
BF = jnp.bfloat16
F32 = jnp.float32
MESH = pl.DeviceIdType.MESH
GROUP = 16
LANES = 128


def run_column(levels_ref, index, p):
    col = index[:, p : p + 1]
    out = jnp.zeros(col.shape, F32)
    for level in range(levels_ref.shape[1]):
        out = jnp.where(col == level, levels_ref[p, level], out)
    return out


def stencil_kernel(
    n_strip, levels, index, base, material, out,
    bx, mx, u_a, u_b, k_a, k_b, cond, cond_g, shots,
    local_sem, halo_send, halo_recv, keep_sem, send_sem, recv_sem,
):
    rows_x, nz, ny = base.shape
    ext = rows_x + 2 * STEPS
    run = lax.axis_index("run")
    strip = lax.axis_index("strip")
    core = lax.rem(run, 2)
    slab = lax.div(run, 2)
    partner = run + 1 - 2 * core
    right = lax.rem(strip + 1, n_strip)
    left = lax.rem(strip + n_strip - 1, n_strip)

    local = [
        pltpu.make_async_copy(src, dst.at[pl.ds(STEPS, rows_x)], local_sem.at[i])
        for i, (src, dst) in enumerate(((base, bx), (material, mx)))
    ]
    for copy in local:
        copy.start()
    barrier = pltpu.get_barrier_semaphore()
    for where in ({"strip": left}, {"strip": right}, {"run": partner}):
        pl.semaphore_signal(barrier, inc=1, device_id=where, device_id_type=MESH)
    pl.semaphore_wait(barrier, 3)
    halos = []
    for i, (src, dst) in enumerate(((base, bx), (material, mx))):
        for j, (first, to, target) in enumerate(
            ((rows_x - STEPS, 0, right), (0, STEPS + rows_x, left))
        ):
            copy = pltpu.make_async_remote_copy(
                src_ref=src.at[pl.ds(first, STEPS)],
                dst_ref=dst.at[pl.ds(to, STEPS)],
                send_sem=halo_send.at[2 * i + j],
                recv_sem=halo_recv.at[2 * i + j],
                device_id={"strip": target},
                device_id_type=MESH,
            )
            copy.start()
            halos.append(copy)

    zero_row = jnp.zeros((GROUP, ny), BF)

    def clear(pad):
        def body(x, carry):
            for ref in (u_a, u_b, k_a, k_b):
                ref[pad, x] = zero_row
            return carry

        lax.fori_loop(0, ext, body, 0)

    clear(0)
    clear(nz + 1)
    for copy in local:
        copy.wait()

    lane = lax.broadcasted_iota(jnp.int32, (GROUP, LANES), 1).astype(F32).astype(BF)
    first_lane = lane == jnp.asarray(0, BF)
    last_lane = lane == jnp.asarray(LANES - 1, BF)
    zero = jnp.zeros((GROUP, LANES), BF)

    def prepare(g):
        picks = index[pl.ds(pl.multiple_of(core * 2 * GROUP + g * GROUP, GROUP), GROUP), :]
        vals = [run_column(levels, picks, p) for p in range(6)]
        wide = lambda col: jnp.broadcast_to(col, (GROUP, LANES))
        kinds = [wide(0.5 * TIME_STEP * vals[m]).astype(BF) for m in range(4)]
        growth = 0.1 * vals[4]
        kinds_g = [wide(0.5 * TIME_STEP * vals[m] * growth).astype(BF) for m in range(4)]
        start = wide(vals[5])
        return kinds, kinds_g, start

    def fill(first, count, unroll, kinds, kinds_g, start):
        def one(x):
            tile = bx[x]
            mats = mx[x].astype(F32)
            for z in range(nz):
                for h in range(2):
                    cut = slice(h * LANES, (h + 1) * LANES)
                    mat = jnp.broadcast_to(mats[z : z + 1, cut], (GROUP, LANES)).astype(BF)
                    c, cg = kinds[0], kinds_g[0]
                    for m in range(1, 4):
                        hit = mat == jnp.asarray(m, BF)
                        c = jnp.where(hit, kinds[m], c)
                        cg = jnp.where(hit, kinds_g[m], cg)
                    u = (jnp.broadcast_to(tile[z : z + 1, cut], (GROUP, LANES)) * start).astype(BF)
                    cond[z, x, :, cut] = c
                    cond_g[z, x, :, cut] = cg
                    u_a[z + 1, x, :, cut] = u
                    k_a[z + 1, x, :, cut] = c + cg * (u * u)

        def body(i, carry):
            for j in range(unroll):
                one(first + i * unroll + j)
            return carry

        lax.fori_loop(0, count // unroll, body, 0)

    def blank(refs, first, count):
        def body(z, carry):
            for x in range(first, first + count):
                for ref, shift in refs:
                    ref[z + shift, x] = zero_row
            return carry

        lax.fori_loop(0, nz, body, 0)

    def advance(step, g, us, ks, ud, kd):
        rows = ext - 2 * step
        unroll = {70: 14, 68: 17, 66: 22, 64: 16}.get(rows, 1)
        reach = STEPS - step
        final = step == STEPS
        low = jnp.maximum(slab - reach, 0)
        high = jnp.minimum(slab + reach, nz - 1)

        def slab_body(z, carry):
            zp = z + 1

            def halves(ref, a, x):
                row = ref[a, x]
                return [row[:, :LANES], row[:, LANES:]]

            u0, k0 = halves(us, zp, step), halves(ks, zp, step)
            ub, kb = halves(us, zp, step - 1), halves(ks, zp, step - 1)
            fl0 = [(k0[h] + kb[h]) * (u0[h] - ub[h]) for h in range(2)]

            def cell(x, u, k, fl):
                un, kn = halves(us, zp, x + 1), halves(ks, zp, x + 1)
                uu, ku = halves(us, zp + 1, x), halves(ks, zp + 1, x)
                ul, kl = halves(us, zp - 1, x), halves(ks, zp - 1, x)
                ru = [pltpu.roll(v, LANES - 1, 1) for v in u]
                rk = [pltpu.roll(v, LANES - 1, 1) for v in k]
                up = [jnp.where(last_lane, ru[1], ru[0]), jnp.where(last_lane, zero, ru[1])]
                kp = [jnp.where(last_lane, rk[1], rk[0]), jnp.where(last_lane, zero, rk[1])]
                fy = [(k[h] + kp[h]) * (up[h] - u[h]) for h in range(2)]
                rf = [pltpu.roll(v, 1, 1) for v in fy]
                fyl = [jnp.where(first_lane, k[0] * u[0], rf[0]), jnp.where(first_lane, rf[0], rf[1])]
                fr = []
                for h in range(2):
                    face = (k[h] + kn[h]) * (un[h] - u[h])
                    top = (k[h] + ku[h]) * (uu[h] - u[h])
                    low_face = (k[h] + kl[h]) * (u[h] - ul[h])
                    total = (face - fl[h]) + (top - low_face) + (fy[h] - fyl[h])
                    new = u[h] + total
                    cut = slice(h * LANES, (h + 1) * LANES)
                    if final:
                        shots[h, step - 1, g, x - STEPS] = new
                    else:
                        ud[zp, x, :, cut] = new
                        kd[zp, x, :, cut] = cond[z, x, :, cut] + cond_g[z, x, :, cut] * (new * new)
                    fr.append(face)
                return un, kn, fr

            def body(i, carry):
                u, k, fl = carry
                for j in range(unroll):
                    u, k, fl = cell(step + i * unroll + j, u, k, fl)
                return u, k, fl

            lax.fori_loop(0, rows // unroll, body, (u0, k0, fl0))
            return carry

        lax.fori_loop(low, high + 1, slab_body, 0)
        if not final:

            @pl.when(strip == 0)
            def _():
                blank([(ud, 1)], 0, STEPS)

            @pl.when(strip == n_strip - 1)
            def _():
                blank([(ud, 1)], STEPS + rows_x, STEPS)

            def keep(i, carry):
                for j in range(8):
                    x = i * 8 + j
                    for h in range(2):
                        shots[h, step - 1, g, x] = ud[slab + 1, x + STEPS, :, h * LANES : (h + 1) * LANES]
                return carry

            lax.fori_loop(0, rows_x // 8, keep, 0)

    def sends(step, g):
        mine = pltpu.make_async_copy(
            shots.at[core, step - 1, g], out.at[core, step - 1, g], keep_sem.at[step - 1, g]
        )
        away = pltpu.make_async_remote_copy(
            src_ref=shots.at[1 - core, step - 1, g],
            dst_ref=out.at[core, step - 1, g],
            send_sem=send_sem.at[step - 1, g],
            recv_sem=recv_sem.at[step - 1, g],
            device_id={"run": partner},
            device_id_type=MESH,
        )
        return mine, away

    def group(g, carry):
        consts = prepare(g)
        fill(STEPS, rows_x, 2, *consts)

        @pl.when(g == 0)
        def _():
            for copy in halos:
                copy.wait()

        fill(0, STEPS, 2, *consts)
        fill(STEPS + rows_x, STEPS, 2, *consts)
        everywhere = [(cond, 0), (cond_g, 0), (u_a, 1), (k_a, 1)]

        @pl.when(strip == 0)
        def _():
            blank(everywhere, 0, STEPS)

        @pl.when(strip == n_strip - 1)
        def _():
            blank(everywhere, STEPS + rows_x, STEPS)

        pairs = [(u_a, k_a), (u_b, k_b)]
        for step in range(1, STEPS + 1):
            src, dst = pairs[(step - 1) % 2], pairs[step % 2]
            advance(step, g, *src, *dst)
            for copy in sends(step, g):
                copy.start()
        return carry

    lax.fori_loop(0, 2, group, 0)
    for g in range(2):
        for step in range(1, STEPS + 1):
            for copy in sends(step, g):
                copy.wait()


def snapshots(levels, index, base, material, n_strip):
    rows_x, nz, ny = base.shape
    ext = rows_x + 2 * STEPS
    hbm = pl.BlockSpec(memory_space=pl.ANY)
    field = pltpu.VMEM((nz + 2, ext, GROUP, ny), BF)
    inner = pltpu.VMEM((nz, ext, GROUP, ny), BF)
    return pl.pallas_call(
        functools.partial(stencil_kernel, n_strip),
        out_shape=jax.ShapeDtypeStruct((2, STEPS, 2, rows_x, GROUP, LANES), BF),
        in_specs=[
            pl.BlockSpec(memory_space=pltpu.SMEM),
            pl.BlockSpec(memory_space=pltpu.VMEM),
            hbm,
            hbm,
        ],
        out_specs=hbm,
        scratch_shapes=[
            pltpu.VMEM((ext, nz, ny), F32),
            pltpu.VMEM((ext, nz, ny), jnp.int32),
            field, field, field, field, inner, inner,
            pltpu.VMEM((2, STEPS, 2, rows_x, GROUP, LANES), BF),
            pltpu.SemaphoreType.DMA((2,)),
            pltpu.SemaphoreType.DMA((4,)),
            pltpu.SemaphoreType.DMA((4,)),
            pltpu.SemaphoreType.DMA((STEPS, 2)),
            pltpu.SemaphoreType.DMA((STEPS, 2)),
            pltpu.SemaphoreType.DMA((STEPS, 2)),
        ],
        compiler_params=pltpu.CompilerParams(
            collective_id=0, has_side_effects=True, vmem_limit_bytes=63 * 1024 * 1024
        ),
        name="snapshots",
    )(levels, index, base, material)


def training_kernel(levels, index, w_in, weight, target, grad, partial, hid, hid_b, hid_t, back):
    step = pl.program_id(0)
    half = 2 * GROUP
    units, width, _ = weight.shape
    batch = hid.shape[0]

    @pl.when(step == 0)
    def _():
        picks = index[...]
        total = jnp.zeros((picks.shape[0], units), F32)
        for p in range(6):
            total = total + run_column(levels, picks, p) * w_in[p : p + 1, :]
        for core in range(2):
            for t in range(STEPS):
                rows = total[core * half : (core + 1) * half]
                pre = rows + ((t + 1.0) / STEPS) * w_in[6:7, :] + w_in[7:8, :]
                hid[pl.ds((core * STEPS + t) * half, half), :] = jnp.tanh(pre)
        hid_b[...] = hid[...].astype(BF)
        hid_t[...] = hid[...].T.astype(BF)
        back[...] = jnp.zeros_like(back)

    w = jnp.swapaxes(weight[...], 0, 1)
    w = jnp.concatenate([w[x] for x in range(width)], axis=1)
    pred = jnp.dot(hid_b[...], w, preferred_element_type=F32)
    goal = jnp.concatenate(
        [target[:, :, :, x].reshape(batch, LANES) for x in range(width)], axis=1
    )
    error = ((pred - goal.astype(F32)) * (batch ** -0.5)).astype(BF)
    g = jnp.dot(hid_t[...], error, preferred_element_type=F32).astype(BF)
    g = jnp.stack([g[:, x * LANES : (x + 1) * LANES] for x in range(width)], axis=0)
    grad[...] = jnp.swapaxes(g, 0, 1)
    back[...] += lax.dot_general(error, w, (((1,), (1,)), ((), ())), preferred_element_type=F32)

    @pl.when(step == pl.num_programs(0) - 1)
    def _():
        picks = index[...]
        h = hid[...]
        slope = back[...] * (1.0 - h * h)
        by_step = [
            jnp.concatenate(
                [slope[(core * STEPS + t) * half : (core * STEPS + t + 1) * half] for core in range(2)],
                axis=0,
            )
            for t in range(STEPS)
        ]
        runs = by_step[0] + by_step[1] + by_step[2] + by_step[3]
        rows = [jnp.sum(run_column(levels, picks, p) * runs, axis=0, keepdims=True) for p in range(6)]
        timed = sum(((t + 1.0) / STEPS) * by_step[t] for t in range(STEPS))
        rows.append(jnp.sum(timed, axis=0, keepdims=True))
        rows.append(jnp.sum(runs, axis=0, keepdims=True))
        full = jnp.concatenate(rows, axis=0)
        for q in range(units // LANES):
            partial[q] = full[:, q * LANES : (q + 1) * LANES]


def training(levels, index, w_in, weight, target):
    units, rows_x, _ = weight.shape
    width = 8
    batch = STEPS * index.shape[0]
    vmem = pl.BlockSpec(memory_space=pltpu.VMEM)
    return pl.pallas_call(
        training_kernel,
        grid=(rows_x // width,),
        out_shape=(
            jax.ShapeDtypeStruct(weight.shape, BF),
            jax.ShapeDtypeStruct((units // LANES, 8, LANES), F32),
        ),
        in_specs=[
            pl.BlockSpec(memory_space=pltpu.SMEM),
            vmem,
            vmem,
            pl.BlockSpec((units, width, LANES), lambda i: (0, i, 0)),
            pl.BlockSpec((2, STEPS, 2, width, GROUP, LANES), lambda i: (0, 0, 0, i, 0, 0)),
        ],
        out_specs=(
            pl.BlockSpec((units, width, LANES), lambda i: (0, i, 0)),
            pl.BlockSpec((units // LANES, 8, LANES), lambda i: (0, 0, 0)),
        ),
        scratch_shapes=[
            pltpu.VMEM((batch, units), F32),
            pltpu.VMEM((batch, units), BF),
            pltpu.VMEM((units, batch), BF),
            pltpu.VMEM((batch, units), F32),
        ],
        compiler_params=pltpu.CompilerParams(
            dimension_semantics=("arbitrary",), vmem_limit_bytes=48 * 1024 * 1024
        ),
        name="training",
    )(levels, index, w_in, weight, target)


def reduce_kernel(n_run, n_strip, partial, out, got_run, mid, got_strip, s_run, r_run, s_strip, r_strip):
    run = lax.axis_index("run")
    strip = lax.axis_index("strip")
    per = LANES // (partial.shape[0] * LANES // n_run)
    barrier = pltpu.get_barrier_semaphore()
    peers = [{"run": lax.rem(run + j, n_run)} for j in range(1, n_run)]
    peers += [{"strip": lax.rem(strip + j, n_strip)} for j in range(1, n_strip)]
    for where in peers:
        pl.semaphore_signal(barrier, inc=1, device_id=where, device_id_type=MESH)
    pl.semaphore_wait(barrier, n_run + n_strip - 2)
    copies = []
    for j in range(1, n_run):
        to = lax.rem(run + j, n_run)
        copies.append(
            pltpu.make_async_remote_copy(
                src_ref=partial.at[lax.div(to, per)],
                dst_ref=got_run.at[j - 1],
                send_sem=s_run.at[j - 1],
                recv_sem=r_run.at[j - 1],
                device_id={"run": to},
                device_id_type=MESH,
            )
        )
        copies[-1].start()
    total = partial[lax.div(run, per)]
    for j in range(n_run - 1):
        copies[j].wait_recv()
        total = total + got_run[j]
    mid[...] = total
    more = []
    for j in range(1, n_strip):
        to = lax.rem(strip + j, n_strip)
        more.append(
            pltpu.make_async_remote_copy(
                src_ref=mid,
                dst_ref=got_strip.at[j - 1],
                send_sem=s_strip.at[j - 1],
                recv_sem=r_strip.at[j - 1],
                device_id={"strip": to},
                device_id_type=MESH,
            )
        )
        more[-1].start()
    for j in range(n_strip - 1):
        more[j].wait_recv()
        total = total + got_strip[j]
    for copy in copies + more:
        copy.wait_send()
    keep = out.shape[1]
    at = lax.rem(run, per) * (n_strip * keep) + strip * keep
    out[...] = pltpu.roll(total, lax.rem(LANES - at, LANES), 1)[:, :keep]


def reduced(partial, n_run, n_strip):
    units = partial.shape[0] * LANES
    vmem = pl.BlockSpec(memory_space=pltpu.VMEM)
    return pl.pallas_call(
        functools.partial(reduce_kernel, n_run, n_strip),
        out_shape=jax.ShapeDtypeStruct((8, units // (n_run * n_strip)), F32),
        in_specs=[vmem],
        out_specs=vmem,
        scratch_shapes=[
            pltpu.VMEM((n_run - 1, 8, LANES), F32),
            pltpu.VMEM((8, LANES), F32),
            pltpu.VMEM((n_strip - 1, 8, LANES), F32),
            pltpu.SemaphoreType.DMA((n_run - 1,)),
            pltpu.SemaphoreType.DMA((n_run - 1,)),
            pltpu.SemaphoreType.DMA((n_strip - 1,)),
            pltpu.SemaphoreType.DMA((n_strip - 1,)),
        ],
        compiler_params=pltpu.CompilerParams(collective_id=1, has_side_effects=True),
        name="reduced",
    )(partial)


def solution(mesh):
    n_run, n_strip = mesh.shape["run"], mesh.shape["strip"]

    def local(base_field, material_map, param_levels, param_index, w_input, w_output):
        target = snapshots(param_levels, param_index, base_field, material_map, n_strip)
        grad_output, partial = training(param_levels, param_index, w_input, w_output, target)
        return grad_output, reduced(partial, n_run, n_strip)

    placed = (
        P("strip", None, None),
        P("strip", None, None),
        P(),
        P(),
        P(),
        P(None, "strip", "run"),
    )
    return jax.shard_map(
        local,
        mesh=mesh,
        in_specs=placed,
        out_specs=(P(None, "strip", "run"), P(None, ("run", "strip"))),
        check_vma=False,
    )
```

```python
import functools

import jax
import jax.numpy as jnp
from jax import lax
from jax.experimental import pallas as pl
from jax.experimental.pallas import tpu as pltpu
from jax.sharding import PartitionSpec as P

STEPS = 4
TIME_STEP = 0.08
BF = jnp.bfloat16
F32 = jnp.float32
MESH = pl.DeviceIdType.MESH
GROUP = 16
LANES = 128
CHUNK = 35
WIDTH = 8


def run_values(levels_ref, index_ref):
    rows = []
    for p in range(index_ref.shape[0]):
        row = index_ref[p : p + 1, :]
        out = jnp.zeros(row.shape, F32)
        for level in range(levels_ref.shape[1]):
            out = jnp.where(row == level, levels_ref[p, level], out)
        rows.append(out)
    rows.append(jnp.zeros((8 - len(rows), index_ref.shape[1]), F32))
    return jnp.concatenate(rows, axis=0).T


def forward_kernel(n_run, n_strip, levels, index, w_in, base, material, weight, *rest):
    rows_x, nz, _ = base.shape
    units = weight.shape[0]
    batch = STEPS * index.shape[1]
    blocks = rows_x // WIDTH
    ext = rows_x + 2 * STEPS
    field = pltpu.VMEM((nz + 2, ext, 2, GROUP, LANES), BF)
    inner = pltpu.VMEM((nz, ext, 2, GROUP, LANES), BF)
    row = pltpu.VMEM((ext, 2, GROUP, LANES), BF)
    pl.run_scoped(
        functools.partial(
            forward_body, n_run, n_strip, levels, index, w_in, base, material, weight, *rest
        ),
        field, field, field, field, inner, inner, row, row, row,
        pltpu.VMEM((2, 2 * LANES, 2 * LANES), BF),
        pltpu.VMEM((blocks, units, WIDTH, LANES), BF),
        pltpu.VMEM((blocks, batch, WIDTH * LANES), BF),
        pltpu.VMEM((index.shape[1], units), F32),
        pltpu.VMEM((batch, units), F32),
        pltpu.VMEM((batch, units), BF),
        pltpu.VMEM((batch, units), F32),
    )


def forward_body(
    n_run, n_strip, levels, index, w_in, base, material, weight,
    error_out, hid_out, grad_out,
    bx, mx, shots, landed, values, partial, got_run, mid, got_strip,
    local_sem, halo_send, halo_recv, send_sem, recv_sem, w_sem, e_sem,
    s_run, r_run, s_strip, r_strip,
    u_a, u_b, k_a, k_b, cond, cond_g, tops, flux_y, flux_next, shifts,
    w_all, e_all, mixed, hid, hid_b, back,
):
    rows_x, nz, ny = base.shape
    ext = rows_x + 2 * STEPS
    run = lax.axis_index("run")
    strip = lax.axis_index("strip")
    core = lax.rem(run, 2)
    slab = lax.div(run, 2)
    partner = run + 1 - 2 * core
    right = lax.rem(strip + 1, n_strip)
    left = lax.rem(strip + n_strip - 1, n_strip)

    local = [
        pltpu.make_async_copy(src, dst.at[pl.ds(STEPS, rows_x)], local_sem.at[i])
        for i, (src, dst) in enumerate(((base, bx), (material, mx)))
    ]
    for copy in local:
        copy.start()
    blocks = rows_x // WIDTH
    fetches = [
        pltpu.make_async_copy(
            weight.at[:, pl.ds(i * WIDTH, WIDTH), :], w_all.at[i], w_sem.at[i]
        )
        for i in range(blocks)
    ]
    barrier = pltpu.get_barrier_semaphore()
    peers = [{"run": lax.rem(run + j, n_run)} for j in range(1, n_run)]
    peers += [{"strip": lax.rem(strip + j, n_strip)} for j in range(1, n_strip)]
    for where in peers:
        pl.semaphore_signal(barrier, inc=1, device_id=where, device_id_type=MESH)
    pl.semaphore_wait(barrier, n_run + n_strip - 2)
    halos = []
    for i, (src, dst) in enumerate(((base, bx), (material, mx))):
        for j, (first, to, target) in enumerate(
            ((rows_x - STEPS, 0, right), (0, STEPS + rows_x, left))
        ):
            copy = pltpu.make_async_remote_copy(
                src_ref=src.at[pl.ds(first, STEPS)],
                dst_ref=dst.at[pl.ds(to, STEPS)],
                send_sem=halo_send.at[2 * i + j],
                recv_sem=halo_recv.at[2 * i + j],
                device_id={"strip": target},
                device_id_type=MESH,
            )
            copy.start()
            halos.append(copy)

    for copy in fetches:
        copy.start()
    zero_row = jnp.zeros((2, GROUP, LANES), BF)
    vals = run_values(levels, index)
    values[...] = vals
    hidden_layer(vals, w_in, core, mixed, hid, hid_b, hid_out)

    def clear(pad):
        def body(x, carry):
            for ref in (u_a, u_b, k_a, k_b):
                ref[pad, x] = zero_row
            return carry

        lax.fori_loop(0, ext, body, 0)

    clear(0)
    clear(nz + 1)
    for copy in local:
        copy.wait()

    lane = lax.broadcasted_iota(jnp.int32, (GROUP, LANES), 1).astype(F32).astype(BF)
    first_lane = lane == jnp.asarray(0, BF)
    way = jnp.where(slab >= nz // 2, -1, 1)
    down = lax.broadcasted_iota(jnp.int32, (ny, ny), 0)
    across = lax.broadcasted_iota(jnp.int32, (ny, ny), 1)
    after = (down == across + 1).astype(F32)
    same = (down == across).astype(F32)
    shifts[0] = (after - same).astype(BF)
    shifts[1] = (after + same).astype(BF)

    def prepare(g):
        mine = values[pl.ds(pl.multiple_of(core * 2 * GROUP + g * GROUP, GROUP), GROUP), :]
        vals = [mine[:, p : p + 1] for p in range(6)]
        wide = lambda col: jnp.broadcast_to(col, (GROUP, LANES))
        kinds = [wide(0.5 * TIME_STEP * vals[m]).astype(BF) for m in range(4)]
        growth = wide(0.1 * vals[4]).astype(BF)
        start = wide(vals[5])
        return kinds, growth, start

    def fill(first, count, unroll, kinds, growth, start):
        def one(x):
            tile = bx[x]
            mats = mx[x].astype(F32)
            for z in range(nz):
                for h in range(2):
                    cut = slice(h * LANES, (h + 1) * LANES)
                    mat = jnp.broadcast_to(mats[z : z + 1, cut], (GROUP, LANES)).astype(BF)
                    c = kinds[0]
                    for m in range(1, 4):
                        c = jnp.where(mat == jnp.asarray(m, BF), kinds[m], c)
                    cg = c * growth
                    u = (jnp.broadcast_to(tile[z : z + 1, cut], (GROUP, LANES)) * start).astype(BF)
                    cond[z, x, h] = c
                    cond_g[z, x, h] = cg
                    u_a[z + 1, x, h] = u
                    k_a[z + 1, x, h] = c + cg * (u * u)

        def body(i, carry):
            for j in range(unroll):
                one(first + i * unroll + j)
            return carry

        lax.fori_loop(0, count // unroll, body, 0)

    def blank(refs, first, count):
        def body(z, carry):
            for x in range(first, first + count):
                for ref, shift in refs:
                    ref[z + shift, x] = zero_row
            return carry

        lax.fori_loop(0, nz, body, 0)

    def halves(ref, a, x):
        return [ref[a, x, 0], ref[a, x, 1]]

    def flat(block):
        count = block.shape[0] * GROUP
        sides = [block[:, h].reshape(count, LANES) for h in range(2)]
        return jnp.concatenate(sides, axis=1)

    def along_y(us, ks, zp, first, count):
        u, k = us[zp, pl.ds(first, count)], ks[zp, pl.ds(first, count)]
        rise = jnp.dot(flat(u), shifts[0], preferred_element_type=F32).astype(BF)
        pair = jnp.dot(flat(k), shifts[1], preferred_element_type=F32).astype(BF)
        face = rise * pair
        out = []
        for j in range(count):
            f = [face[j * GROUP : (j + 1) * GROUP, h * LANES : (h + 1) * LANES] for h in range(2)]
            r = [pltpu.roll(v, 1, 1) for v in f]
            out.append(
                [
                    f[0] - jnp.where(first_lane, k[j, 0] * u[j, 0], r[0]),
                    f[1] - jnp.where(first_lane, r[0], r[1]),
                ]
            )
        return out

    def keep_y(flux, first, ref):
        for j, pair in enumerate(flux):
            for h in range(2):
                ref[first + j, h] = pair[h]

    def chunks(step):
        return [(x, min(CHUNK, ext - step - x)) for x in range(step, ext - step, CHUNK)]

    def span(step):
        reach = STEPS - step
        low = jnp.maximum(slab - reach, 0)
        high = jnp.minimum(slab + reach, nz - 1)
        return jnp.where(way > 0, low, high), high - low + 1

    def start_y(us, ks):
        zp = span(1)[0] + 1
        for first, count in chunks(1):
            keep_y(along_y(us, ks, zp, first, count), first, flux_y)

    def advance(step, g, us, ks, ud, kd):
        final = step == STEPS
        begin, number = span(step)

        def one_slab(z, last):
            zp = z + 1
            after = (span(step + 1)[0] + 1) if last else zp + way
            src = (ud, kd) if last else (us, ks)
            if last and not final:
                for first, count in chunks(step):
                    keep_y(along_y(*src, after, first, count), first, flux_next)
            u, k = halves(us, zp, step), halves(ks, zp, step)
            ub, kb = halves(us, zp, step - 1), halves(ks, zp, step - 1)
            fl = [(k[h] + kb[h]) * (u[h] - ub[h]) for h in range(2)]
            for first, count in chunks(step):
                flux = None if last else along_y(*src, after, first, count)
                for x in range(first, first + count):
                    un, kn = halves(us, zp, x + 1), halves(ks, zp, x + 1)
                    uz, kz = halves(us, zp + way, x), halves(ks, zp + way, x)
                    fr = []
                    for h in range(2):
                        face = (k[h] + kn[h]) * (un[h] - u[h])
                        top = (k[h] + kz[h]) * (uz[h] - u[h])
                        total = (face - fl[h]) + (top - tops[x, h]) + flux_y[x, h]
                        new = u[h] + total
                        if final:
                            shots[h, step - 1, g, x - STEPS] = new
                        else:
                            if not last:
                                tops[x, h] = top
                            ud[zp, x, h] = new
                            kd[zp, x, h] = cond[z, x, h] + cond_g[z, x, h] * (new * new)
                        fr.append(face)
                    u, k, fl = un, kn, fr
                if flux is not None:
                    keep_y(flux, first, flux_y)
            if last and not final:
                for x in range(step, ext - step):
                    for h in range(2):
                        flux_y[x, h] = flux_next[x, h]

        def first_faces(i, carry):
            for j in range(2):
                x = step + i * 2 + j
                for h in range(2):
                    du = us[begin + 1, x, h] - us[begin + 1 - way, x, h]
                    tops[x, h] = (ks[begin + 1, x, h] + ks[begin + 1 - way, x, h]) * du
            return carry

        def slabs(i, carry):
            one_slab(begin + way * i, False)
            return carry

        lax.fori_loop(0, (ext - 2 * step) // 2, first_faces, 0)
        if not final:
            lax.fori_loop(0, number - 1, slabs, 0)
        one_slab(begin + way * (number - 1), True)
        if not final:

            @pl.when(strip == 0)
            def _():
                blank([(ud, 1)], 0, STEPS)

            @pl.when(strip == n_strip - 1)
            def _():
                blank([(ud, 1)], STEPS + rows_x, STEPS)

            def keep(i, carry):
                for j in range(8):
                    x = i * 8 + j
                    for h in range(2):
                        shots[h, step - 1, g, x] = ud[slab + 1, x + STEPS, h]
                return carry

            lax.fori_loop(0, rows_x // 8, keep, 0)

    def send(step, g):
        return pltpu.make_async_remote_copy(
            src_ref=shots.at[1 - core, step - 1, g],
            dst_ref=landed.at[step - 1, g],
            send_sem=send_sem.at[step - 1, g],
            recv_sem=recv_sem.at[step - 1, g],
            device_id={"run": partner},
            device_id_type=MESH,
        )

    def group(g, carry):
        consts = prepare(g)
        fill(STEPS, rows_x, 2, *consts)

        @pl.when(g == 0)
        def _():
            for copy in halos:
                copy.wait()

        fill(0, STEPS, 2, *consts)
        fill(STEPS + rows_x, STEPS, 2, *consts)
        everywhere = [(cond, 0), (cond_g, 0), (u_a, 1), (k_a, 1)]

        @pl.when(strip == 0)
        def _():
            blank(everywhere, 0, STEPS)

        @pl.when(strip == n_strip - 1)
        def _():
            blank(everywhere, STEPS + rows_x, STEPS)

        start_y(u_a, k_a)
        pairs = [(u_a, k_a), (u_b, k_b)]
        for step in range(1, STEPS + 1):
            src, dst = pairs[(step - 1) % 2], pairs[step % 2]
            advance(step, g, *src, *dst)
            send(step, g).start()
        return carry

    lax.fori_loop(0, 2, group, 0)
    for copy in fetches:
        copy.wait()
    back[...] = jnp.zeros_like(back)
    for g in range(2):
        for step in range(1, STEPS + 1):
            send(step, g).wait()

    batch = hid.shape[0]

    def put(i):
        return pltpu.make_async_copy(e_all.at[i], error_out.at[i], e_sem.at[i])

    def train(i, carry):
        w = jnp.swapaxes(w_all[i], 0, 1)
        w = jnp.concatenate([w[x] for x in range(WIDTH)], axis=1)
        pred = jnp.dot(hid_b[...], w, preferred_element_type=F32)
        cuts = []
        for x in range(WIDTH):
            at = i * WIDTH + x
            tiles = [shots[core, t, g, at] for t in range(STEPS) for g in range(2)]
            tiles += [landed[t, g, at] for t in range(STEPS) for g in range(2)]
            cuts.append(jnp.concatenate(tiles, axis=0))
        goal = jnp.concatenate(cuts, axis=1)
        error = ((pred - goal.astype(F32)) * (batch ** -0.5)).astype(BF)
        e_all[i] = error
        put(i).start()
        back[...] += lax.dot_general(
            error, w, (((1,), (1,)), ((), ())), preferred_element_type=F32
        )
        return carry

    lax.fori_loop(0, blocks, train, 0)
    input_gradient(values, core, hid, back, partial)
    reduce_scatter(
        n_run, n_strip, partial, grad_out, got_run, mid, got_strip, s_run, r_run, s_strip, r_strip
    )
    for i in range(blocks):
        put(i).wait()


def hidden_layer(vals, w_in, core, mixed, hid, hid_b, hid_out):
    half = 2 * GROUP
    total = vals[:, 0:1] * w_in[0:1, :]
    for p in range(1, 6):
        total = total + vals[:, p : p + 1] * w_in[p : p + 1, :]
    mixed[...] = total
    for part in range(2):
        owner = core if part == 0 else 1 - core
        rows = mixed[pl.ds(pl.multiple_of(owner * half, half), half), :]
        for t in range(STEPS):
            pre = rows + ((t + 1.0) / STEPS) * w_in[6:7, :] + w_in[7:8, :]
            hid[pl.ds((part * STEPS + t) * half, half), :] = jnp.tanh(pre)
    hid_b[...] = hid[...].astype(BF)
    hid_out[...] = hid[...].T.astype(BF)


def input_gradient(values, core, hid, back, partial):
    half = 2 * GROUP
    h = hid[...]
    slope = back[...] * (1.0 - h * h)
    steps = [
        [slope[(part * STEPS + t) * half : (part * STEPS + t + 1) * half] for t in range(STEPS)]
        for part in range(2)
    ]
    runs = [p[0] + p[1] + p[2] + p[3] for p in steps]
    vals = [
        values[pl.ds(pl.multiple_of((core if part == 0 else 1 - core) * half, half), half), :]
        for part in range(2)
    ]
    rows = []
    for p in range(6):
        both = vals[0][:, p : p + 1] * runs[0] + vals[1][:, p : p + 1] * runs[1]
        rows.append(jnp.sum(both, axis=0, keepdims=True))
    timed = sum(((t + 1.0) / STEPS) * (steps[0][t] + steps[1][t]) for t in range(STEPS))
    rows.append(jnp.sum(timed, axis=0, keepdims=True))
    rows.append(jnp.sum(runs[0] + runs[1], axis=0, keepdims=True))
    full = jnp.concatenate(rows, axis=0)
    for q in range(partial.shape[0]):
        partial[q] = full[:, q * LANES : (q + 1) * LANES]


def reduce_scatter(
    n_run, n_strip, partial, out, got_run, mid, got_strip, s_run, r_run, s_strip, r_strip
):
    run = lax.axis_index("run")
    strip = lax.axis_index("strip")
    units = partial.shape[0] * LANES
    keep = units // (n_run * n_strip)
    per = LANES // (n_strip * keep)
    copies = []
    for j in range(1, n_run):
        to = lax.rem(run + j, n_run)
        copies.append(
            pltpu.make_async_remote_copy(
                src_ref=partial.at[lax.div(to, per)],
                dst_ref=got_run.at[j - 1],
                send_sem=s_run.at[j - 1],
                recv_sem=r_run.at[j - 1],
                device_id={"run": to},
                device_id_type=MESH,
            )
        )
        copies[-1].start()
    total = partial[lax.div(run, per)]
    for j in range(n_run - 1):
        copies[j].wait_recv()
        total = total + got_run[j]
    mid[...] = total
    more = []
    for j in range(1, n_strip):
        to = lax.rem(strip + j, n_strip)
        more.append(
            pltpu.make_async_remote_copy(
                src_ref=mid,
                dst_ref=got_strip.at[j - 1],
                send_sem=s_strip.at[j - 1],
                recv_sem=r_strip.at[j - 1],
                device_id={"strip": to},
                device_id_type=MESH,
            )
        )
        more[-1].start()
    for j in range(n_strip - 1):
        more[j].wait_recv()
        total = total + got_strip[j]
    for copy in copies + more:
        copy.wait_send()
    at = lax.rem(run, per) * (n_strip * keep) + strip * keep
    out[...] = pltpu.roll(total, lax.rem(LANES - at, LANES), 1)


def forward(levels, index, w_in, base, material, weight, n_run, n_strip):
    rows_x, nz, ny = base.shape
    units = weight.shape[0]
    batch = STEPS * index.shape[1]
    blocks = rows_x // WIDTH
    ext = rows_x + 2 * STEPS
    hbm = pl.BlockSpec(memory_space=pl.ANY)
    vmem = pl.BlockSpec(memory_space=pltpu.VMEM)
    dma = pltpu.SemaphoreType.DMA
    return pl.pallas_call(
        functools.partial(forward_kernel, n_run, n_strip),
        out_shape=(
            jax.ShapeDtypeStruct((blocks, batch, WIDTH * LANES), BF),
            jax.ShapeDtypeStruct((units, batch), BF),
            jax.ShapeDtypeStruct((8, LANES), F32),
        ),
        in_specs=[pl.BlockSpec(memory_space=pltpu.SMEM), vmem, vmem, hbm, hbm, hbm],
        out_specs=(hbm, vmem, vmem),
        scratch_shapes=[
            pltpu.VMEM((ext, nz, ny), F32),
            pltpu.VMEM((ext, nz, ny), jnp.int32),
            pltpu.VMEM((2, STEPS, 2, rows_x, GROUP, LANES), BF),
            pltpu.VMEM((STEPS, 2, rows_x, GROUP, LANES), BF),
            pltpu.VMEM((index.shape[1], 8), F32),
            pltpu.VMEM((units // LANES, 8, LANES), F32),
            pltpu.VMEM((n_run - 1, 8, LANES), F32),
            pltpu.VMEM((8, LANES), F32),
            pltpu.VMEM((n_strip - 1, 8, LANES), F32),
            dma((2,)), dma((4,)), dma((4,)), dma((STEPS, 2)), dma((STEPS, 2)),
            dma((blocks,)), dma((blocks,)),
            dma((n_run - 1,)), dma((n_run - 1,)), dma((n_strip - 1,)), dma((n_strip - 1,)),
        ],
        compiler_params=pltpu.CompilerParams(
            collective_id=0, has_side_effects=True, vmem_limit_bytes=63 * 1024 * 1024
        ),
        name="forward",
    )(levels, index, w_in, base, material, weight)


def output_kernel(hid, total, error, grad, turned, e_all, g_all, e_sem, g_sem):
    blocks = e_all.shape[0]
    fetches = [pltpu.make_async_copy(error.at[i], e_all.at[i], e_sem.at[i]) for i in range(blocks)]
    for copy in fetches:
        copy.start()
    turned[...] = total[...].T[: turned.shape[0]]
    puts = []
    for i in range(blocks):
        fetches[i].wait()
        g = jnp.dot(hid[...], e_all[i], preferred_element_type=F32).astype(BF)
        g = jnp.stack([g[:, x * LANES : (x + 1) * LANES] for x in range(WIDTH)], axis=0)
        g_all[i] = jnp.swapaxes(g, 0, 1)
        puts.append(
            pltpu.make_async_copy(
                g_all.at[i], grad.at[:, pl.ds(i * WIDTH, WIDTH), :], g_sem.at[i]
            )
        )
        puts[-1].start()
    for copy in puts:
        copy.wait()


def output_gradient(hid, total, error, keep):
    units, batch = hid.shape
    blocks = error.shape[0]
    hbm = pl.BlockSpec(memory_space=pl.ANY)
    vmem = pl.BlockSpec(memory_space=pltpu.VMEM)
    return pl.pallas_call(
        output_kernel,
        out_shape=(
            jax.ShapeDtypeStruct((units, blocks * WIDTH, LANES), BF),
            jax.ShapeDtypeStruct((keep, 8), F32),
        ),
        in_specs=[vmem, vmem, hbm],
        out_specs=(hbm, vmem),
        scratch_shapes=[
            pltpu.VMEM(error.shape, BF),
            pltpu.VMEM((blocks, units, WIDTH, LANES), BF),
            pltpu.SemaphoreType.DMA((blocks,)),
            pltpu.SemaphoreType.DMA((blocks,)),
        ],
        compiler_params=pltpu.CompilerParams(vmem_limit_bytes=63 * 1024 * 1024),
        name="output_gradient",
    )(hid, total, error)


def solution(mesh):
    n_run, n_strip = mesh.shape["run"], mesh.shape["strip"]

    def local(base_field, material_map, param_levels, param_index, w_input, w_output):
        error, hid, total = forward(
            param_levels, param_index.T, w_input, base_field, material_map, w_output, n_run, n_strip
        )
        keep = w_output.shape[0] // (n_run * n_strip)
        grad_output, turned = output_gradient(hid, total, error, keep)
        return grad_output, turned.T

    placed = (
        P("strip", None, None),
        P("strip", None, None),
        P(),
        P(),
        P(),
        P(None, "strip", "run"),
    )
    return jax.shard_map(
        local,
        mesh=mesh,
        in_specs=placed,
        out_specs=(P(None, "strip", "run"), P(None, ("run", "strip"))),
        check_vma=False,
    )
```

```python
import functools

import jax
import jax.numpy as jnp
from jax import lax
from jax.experimental import pallas as pl
from jax.experimental.pallas import tpu as pltpu
from jax.sharding import PartitionSpec as P

STEPS = 4
TIME_STEP = 0.08
BF = jnp.bfloat16
F32 = jnp.float32
MESH = pl.DeviceIdType.MESH
GROUP = 16
LANES = 128
CHUNK = 35
WIDTH = 8
TURN = 2


def run_values(levels_ref, index_ref):
    rows = []
    for p in range(index_ref.shape[0]):
        row = index_ref[p : p + 1, :]
        out = jnp.zeros(row.shape, F32)
        for level in range(levels_ref.shape[1]):
            out = jnp.where(row == level, levels_ref[p : p + 1, level : level + 1], out)
        rows.append(out)
    rows.append(jnp.zeros((8 - len(rows), index_ref.shape[1]), F32))
    return jnp.concatenate(rows, axis=0).T


def forward_kernel(n_run, n_strip, levels_in, index_in, w_in_in, base, material, weight, *rest):
    rows_x, nz, _ = base.shape
    units = weight.shape[0]
    batch = STEPS * index_in.shape[1]
    blocks = rows_x // WIDTH
    ext = rows_x + 2 * STEPS
    field = pltpu.VMEM((nz + 2, ext, 2, GROUP, LANES), BF)
    inner = pltpu.VMEM((nz, ext, 2, GROUP, LANES), BF)
    row = pltpu.VMEM((ext, 2, GROUP, LANES), BF)
    pl.run_scoped(
        functools.partial(
            forward_body, n_run, n_strip, levels_in, index_in, w_in_in, base, material, weight, *rest
        ),
        field, field, field, field, inner, inner, row, row, row,
        pltpu.VMEM((2, 2 * LANES, 2 * LANES), BF),
        pltpu.VMEM((blocks, units, WIDTH, LANES), BF),
        pltpu.VMEM((blocks, batch, WIDTH * LANES), BF),
        pltpu.VMEM((index_in.shape[1], units), F32),
        pltpu.VMEM((batch, units), F32),
        pltpu.VMEM((batch, units), BF),
        pltpu.VMEM((units, batch), BF),
        pltpu.VMEM((batch, units), F32),
        pltpu.VMEM(levels_in.shape, F32),
        pltpu.VMEM(index_in.shape, jnp.int32),
        pltpu.VMEM(w_in_in.shape, F32),
    )


def forward_body(
    n_run, n_strip, levels_in, index_in, w_in_in, base, material, weight,
    error_out, hid_out, grad_out,
    bx, mx, shots, landed, values, partial, got_run, mid, got_strip,
    local_sem, small_sem, halo_send, halo_recv, send_sem, recv_sem, w_sem, e_sem,
    s_run, r_run, s_strip, r_strip,
    u_a, u_b, k_a, k_b, cond, cond_g, tops, flux_y, flux_next, shifts,
    w_all, e_all, mixed, hid, hid_b, hid_t, back, levels, index, w_in,
):
    rows_x, nz, ny = base.shape
    ext = rows_x + 2 * STEPS
    run = lax.axis_index("run")
    strip = lax.axis_index("strip")
    core = lax.rem(run, 2)
    slab = lax.div(run, 2)
    partner = run + 1 - 2 * core
    right = lax.rem(strip + 1, n_strip)
    left = lax.rem(strip + n_strip - 1, n_strip)

    local = [
        pltpu.make_async_copy(src, dst.at[pl.ds(STEPS, rows_x)], local_sem.at[i])
        for i, (src, dst) in enumerate(((base, bx), (material, mx)))
    ]
    small = [
        pltpu.make_async_copy(src, dst, small_sem.at[i])
        for i, (src, dst) in enumerate(((levels_in, levels), (index_in, index), (w_in_in, w_in)))
    ]
    for copy in small + local:
        copy.start()
    blocks = rows_x // WIDTH
    fetches = [
        pltpu.make_async_copy(
            weight.at[:, pl.ds(i * WIDTH, WIDTH), :], w_all.at[i], w_sem.at[i]
        )
        for i in range(blocks)
    ]
    barrier = pltpu.get_barrier_semaphore()
    peers = [{"run": lax.rem(run + j, n_run)} for j in range(1, n_run)]
    peers += [{"strip": lax.rem(strip + j, n_strip)} for j in range(1, n_strip)]
    for where in peers:
        pl.semaphore_signal(barrier, inc=1, device_id=where, device_id_type=MESH)
    halos = []
    for i, (src, dst) in enumerate(((base, bx), (material, mx))):
        for j, (first, to, target) in enumerate(
            ((rows_x - STEPS, 0, right), (0, STEPS + rows_x, left))
        ):
            halos.append(
                pltpu.make_async_remote_copy(
                    src_ref=src.at[pl.ds(first, STEPS)],
                    dst_ref=dst.at[pl.ds(to, STEPS)],
                    send_sem=halo_send.at[2 * i + j],
                    recv_sem=halo_recv.at[2 * i + j],
                    device_id={"strip": target},
                    device_id_type=MESH,
                )
            )
    hid_put = pltpu.make_async_copy(hid_t, hid_out, small_sem.at[3])
    zero_row = jnp.zeros((2, GROUP, LANES), BF)

    def clear(pad):
        def body(x, carry):
            for ref in (u_a, u_b, k_a, k_b):
                ref[pad, x] = zero_row
            return carry

        lax.fori_loop(0, ext, body, 0)

    clear(0)
    clear(nz + 1)
    for copy in small:
        copy.wait()
    vals = run_values(levels, index)
    values[...] = vals

    lane = lax.broadcasted_iota(jnp.int32, (GROUP, LANES), 1).astype(F32).astype(BF)
    first_lane = lane == jnp.asarray(0, BF)
    way = jnp.where(slab >= nz // 2, -1, 1)
    down = lax.broadcasted_iota(jnp.int32, (ny, ny), 0)
    across = lax.broadcasted_iota(jnp.int32, (ny, ny), 1)
    after = (down == across + 1).astype(F32)
    same = (down == across).astype(F32)
    shifts[0] = (after - same).astype(BF)
    shifts[1] = (after + same).astype(BF)

    def prepare(g):
        mine = values[pl.ds(pl.multiple_of(core * 2 * GROUP + g * GROUP, GROUP), GROUP), :]
        vals = [mine[:, p : p + 1] for p in range(6)]
        wide = lambda col: jnp.broadcast_to(col, (GROUP, LANES))
        kinds = [wide(0.5 * TIME_STEP * vals[m]).astype(BF) for m in range(4)]
        growth = wide(0.1 * vals[4]).astype(BF)
        start = wide(vals[5])
        return kinds, growth, start

    def fill(first, count, unroll, kinds, growth, start):
        def one(x):
            tile = bx[x]
            mats = mx[x].astype(F32)
            for z in range(nz):
                for h in range(2):
                    cut = slice(h * LANES, (h + 1) * LANES)
                    mat = jnp.broadcast_to(mats[z : z + 1, cut], (GROUP, LANES)).astype(BF)
                    c = kinds[0]
                    for m in range(1, 4):
                        c = jnp.where(mat == jnp.asarray(m, BF), kinds[m], c)
                    cg = c * growth
                    u = (jnp.broadcast_to(tile[z : z + 1, cut], (GROUP, LANES)) * start).astype(BF)
                    cond[z, x, h] = c
                    cond_g[z, x, h] = cg
                    u_a[z + 1, x, h] = u
                    k_a[z + 1, x, h] = c + cg * (u * u)

        def body(i, carry):
            for j in range(unroll):
                one(first + i * unroll + j)
            return carry

        lax.fori_loop(0, count // unroll, body, 0)

    def blank(refs, first, count):
        def body(z, carry):
            for x in range(first, first + count):
                for ref, shift in refs:
                    ref[z + shift, x] = zero_row
            return carry

        lax.fori_loop(0, nz, body, 0)

    def halves(ref, a, x):
        return [ref[a, x, 0], ref[a, x, 1]]

    def flat(block):
        count = block.shape[0] * GROUP
        sides = [block[:, h].reshape(count, LANES) for h in range(2)]
        return jnp.concatenate(sides, axis=1)

    def along_y(us, ks, zp, first, count):
        u, k = us[zp, pl.ds(first, count)], ks[zp, pl.ds(first, count)]
        rise = jnp.dot(flat(u), shifts[0], preferred_element_type=F32).astype(BF)
        pair = jnp.dot(flat(k), shifts[1], preferred_element_type=F32).astype(BF)
        face = rise * pair
        out = []
        for j in range(count):
            f = [face[j * GROUP : (j + 1) * GROUP, h * LANES : (h + 1) * LANES] for h in range(2)]
            r = [pltpu.roll(v, 1, 1) for v in f]
            out.append(
                [
                    f[0] - jnp.where(first_lane, k[j, 0] * u[j, 0], r[0]),
                    f[1] - jnp.where(first_lane, r[0], r[1]),
                ]
            )
        return out

    def keep_y(flux, first, ref):
        for j, pair in enumerate(flux):
            for h in range(2):
                ref[first + j, h] = pair[h]

    def chunks(step):
        return [(x, min(CHUNK, ext - step - x)) for x in range(step, ext - step, CHUNK)]

    def span(step):
        reach = STEPS - step
        low = jnp.maximum(slab - reach, 0)
        high = jnp.minimum(slab + reach, nz - 1)
        return jnp.where(way > 0, low, high), high - low + 1

    def start_y(us, ks):
        zp = span(1)[0] + 1
        for first, count in chunks(1):
            keep_y(along_y(us, ks, zp, first, count), first, flux_y)

    def advance(step, g, us, ks, ud, kd):
        final = step == STEPS
        begin, number = span(step)

        def one_slab(z, last):
            zp = z + 1
            after = (span(step + 1)[0] + 1) if last else zp + way
            src = (ud, kd) if last else (us, ks)
            if last and not final:
                for first, count in chunks(step):
                    keep_y(along_y(*src, after, first, count), first, flux_next)
            u, k = halves(us, zp, step), halves(ks, zp, step)
            ub, kb = halves(us, zp, step - 1), halves(ks, zp, step - 1)
            fl = [(k[h] + kb[h]) * (u[h] - ub[h]) for h in range(2)]
            for first, count in chunks(step):
                flux = None if last else along_y(*src, after, first, count)
                for x in range(first, first + count):
                    un, kn = halves(us, zp, x + 1), halves(ks, zp, x + 1)
                    uz, kz = halves(us, zp + way, x), halves(ks, zp + way, x)
                    fr = []
                    for h in range(2):
                        face = (k[h] + kn[h]) * (un[h] - u[h])
                        top = (k[h] + kz[h]) * (uz[h] - u[h])
                        total = (face - fl[h]) + (top - tops[x, h]) + flux_y[x, h]
                        new = u[h] + total
                        if final:
                            shots[h, step - 1, g, x - STEPS] = new
                        else:
                            if not last:
                                tops[x, h] = top
                            ud[zp, x, h] = new
                            kd[zp, x, h] = cond[z, x, h] + cond_g[z, x, h] * (new * new)
                        fr.append(face)
                    u, k, fl = un, kn, fr
                if flux is not None:
                    keep_y(flux, first, flux_y)
            if last and not final:
                for x in range(step, ext - step):
                    for h in range(2):
                        flux_y[x, h] = flux_next[x, h]

        def first_faces(i, carry):
            for j in range(2):
                x = step + i * 2 + j
                for h in range(2):
                    du = us[begin + 1, x, h] - us[begin + 1 - way, x, h]
                    tops[x, h] = (ks[begin + 1, x, h] + ks[begin + 1 - way, x, h]) * du
            return carry

        def slabs(i, carry):
            one_slab(begin + way * i, False)
            return carry

        lax.fori_loop(0, (ext - 2 * step) // 2, first_faces, 0)
        if not final:
            lax.fori_loop(0, number - 1, slabs, 0)
        one_slab(begin + way * (number - 1), True)
        if not final:

            @pl.when(strip == 0)
            def _():
                blank([(ud, 1)], 0, STEPS)

            @pl.when(strip == n_strip - 1)
            def _():
                blank([(ud, 1)], STEPS + rows_x, STEPS)

            def keep(i, carry):
                for j in range(8):
                    x = i * 8 + j
                    for h in range(2):
                        shots[h, step - 1, g, x] = ud[slab + 1, x + STEPS, h]
                return carry

            lax.fori_loop(0, rows_x // 8, keep, 0)

    def send(step, g):
        return pltpu.make_async_remote_copy(
            src_ref=shots.at[1 - core, step - 1, g],
            dst_ref=landed.at[step - 1, g],
            send_sem=send_sem.at[step - 1, g],
            recv_sem=recv_sem.at[step - 1, g],
            device_id={"run": partner},
            device_id_type=MESH,
        )

    def group(g, carry):
        @pl.when(g > 0)
        def _():
            fill(0, ext, 2, *prepare(g))

        everywhere = [(cond, 0), (cond_g, 0), (u_a, 1), (k_a, 1)]

        @pl.when(strip == 0)
        def _():
            blank(everywhere, 0, STEPS)

        @pl.when(strip == n_strip - 1)
        def _():
            blank(everywhere, STEPS + rows_x, STEPS)

        start_y(u_a, k_a)
        pairs = [(u_a, k_a), (u_b, k_b)]
        for step in range(1, STEPS + 1):
            src, dst = pairs[(step - 1) % 2], pairs[step % 2]
            advance(step, g, *src, *dst)
            send(step, g).start()
        return carry

    consts = prepare(0)
    for copy in local:
        copy.wait()
    fill(STEPS, rows_x // 2, 2, *consts)
    pl.semaphore_wait(barrier, n_run + n_strip - 2)
    for copy in halos + fetches:
        copy.start()
    fill(STEPS + rows_x // 2, rows_x // 2, 2, *consts)
    hidden_layer(vals, w_in, core, mixed, hid, hid_b, hid_t)
    hid_put.start()
    for copy in halos:
        copy.wait()
    fill(0, STEPS, 2, *consts)
    fill(STEPS + rows_x, STEPS, 2, *consts)
    lax.fori_loop(0, 2, group, 0)
    for copy in fetches:
        copy.wait()
    back[...] = jnp.zeros_like(back)
    for g in range(2):
        for step in range(1, STEPS + 1):
            send(step, g).wait()

    batch = hid.shape[0]

    def put(i):
        return pltpu.make_async_copy(e_all.at[i], error_out.at[i], e_sem.at[i])

    def train(i):
        w = jnp.swapaxes(w_all[i], 0, 1)
        w = jnp.concatenate([w[x] for x in range(WIDTH)], axis=1)
        pred = jnp.dot(hid_b[...], w, preferred_element_type=F32)
        cuts = []
        for x in range(WIDTH):
            at = i * WIDTH + x
            tiles = [shots[core, t, g, at] for t in range(STEPS) for g in range(2)]
            tiles += [landed[t, g, at] for t in range(STEPS) for g in range(2)]
            cuts.append(jnp.concatenate(tiles, axis=0))
        goal = jnp.concatenate(cuts, axis=1)
        error = ((pred - goal.astype(F32)) * (batch ** -0.5)).astype(BF)
        e_all[i] = error
        put(i).start()
        return lax.dot_general(error, w, (((1,), (1,)), ((), ())), preferred_element_type=F32)

    def several(i, carry):
        back[...] += sum(train(i * TURN + j) for j in range(TURN))
        return carry

    lax.fori_loop(0, blocks // TURN, several, 0)
    input_gradient(values, core, hid, back, partial)
    reduce_scatter(
        n_run, n_strip, partial, grad_out, got_run, mid, got_strip, s_run, r_run, s_strip, r_strip
    )
    hid_put.wait()
    for i in range(blocks):
        put(i).wait()


def hidden_layer(vals, w_in, core, mixed, hid, hid_b, hid_t):
    half = 2 * GROUP
    total = vals[:, 0:1] * w_in[0:1, :]
    for p in range(1, 6):
        total = total + vals[:, p : p + 1] * w_in[p : p + 1, :]
    mixed[...] = total
    for part in range(2):
        owner = core if part == 0 else 1 - core
        rows = mixed[pl.ds(pl.multiple_of(owner * half, half), half), :]
        for t in range(STEPS):
            pre = rows + ((t + 1.0) / STEPS) * w_in[6:7, :] + w_in[7:8, :]
            hid[pl.ds((part * STEPS + t) * half, half), :] = jnp.tanh(pre)
    hid_b[...] = hid[...].astype(BF)
    hid_t[...] = hid[...].T.astype(BF)


def input_gradient(values, core, hid, back, partial):
    half = 2 * GROUP
    h = hid[...]
    slope = back[...] * (1.0 - h * h)
    steps = [
        [slope[(part * STEPS + t) * half : (part * STEPS + t + 1) * half] for t in range(STEPS)]
        for part in range(2)
    ]
    runs = [p[0] + p[1] + p[2] + p[3] for p in steps]
    vals = [
        values[pl.ds(pl.multiple_of((core if part == 0 else 1 - core) * half, half), half), :]
        for part in range(2)
    ]
    rows = []
    for p in range(6):
        both = vals[0][:, p : p + 1] * runs[0] + vals[1][:, p : p + 1] * runs[1]
        rows.append(jnp.sum(both, axis=0, keepdims=True))
    timed = sum(((t + 1.0) / STEPS) * (steps[0][t] + steps[1][t]) for t in range(STEPS))
    rows.append(jnp.sum(timed, axis=0, keepdims=True))
    rows.append(jnp.sum(runs[0] + runs[1], axis=0, keepdims=True))
    full = jnp.concatenate(rows, axis=0)
    for q in range(partial.shape[0]):
        partial[q] = full[:, q * LANES : (q + 1) * LANES]


def reduce_scatter(
    n_run, n_strip, partial, out, got_run, mid, got_strip, s_run, r_run, s_strip, r_strip
):
    run = lax.axis_index("run")
    strip = lax.axis_index("strip")
    units = partial.shape[0] * LANES
    keep = units // (n_run * n_strip)
    per = LANES // (n_strip * keep)
    copies = []
    for j in range(1, n_run):
        to = lax.rem(run + j, n_run)
        copies.append(
            pltpu.make_async_remote_copy(
                src_ref=partial.at[lax.div(to, per)],
                dst_ref=got_run.at[j - 1],
                send_sem=s_run.at[j - 1],
                recv_sem=r_run.at[j - 1],
                device_id={"run": to},
                device_id_type=MESH,
            )
        )
        copies[-1].start()
    total = partial[lax.div(run, per)]
    for j in range(n_run - 1):
        copies[j].wait_recv()
        total = total + got_run[j]
    mid[...] = total
    more = []
    for j in range(1, n_strip):
        to = lax.rem(strip + j, n_strip)
        more.append(
            pltpu.make_async_remote_copy(
                src_ref=mid,
                dst_ref=got_strip.at[j - 1],
                send_sem=s_strip.at[j - 1],
                recv_sem=r_strip.at[j - 1],
                device_id={"strip": to},
                device_id_type=MESH,
            )
        )
        more[-1].start()
    for j in range(n_strip - 1):
        more[j].wait_recv()
        total = total + got_strip[j]
    for copy in copies + more:
        copy.wait_send()
    at = lax.rem(run, per) * (n_strip * keep) + strip * keep
    out[...] = pltpu.roll(total, lax.rem(LANES - at, LANES), 1)


def forward(levels, index, w_in, base, material, weight, n_run, n_strip):
    rows_x, nz, ny = base.shape
    units = weight.shape[0]
    batch = STEPS * index.shape[1]
    blocks = rows_x // WIDTH
    ext = rows_x + 2 * STEPS
    hbm = pl.BlockSpec(memory_space=pl.ANY)
    vmem = pl.BlockSpec(memory_space=pltpu.VMEM)
    dma = pltpu.SemaphoreType.DMA
    return pl.pallas_call(
        functools.partial(forward_kernel, n_run, n_strip),
        out_shape=(
            jax.ShapeDtypeStruct((blocks, batch, WIDTH * LANES), BF),
            jax.ShapeDtypeStruct((units, batch), BF),
            jax.ShapeDtypeStruct((8, LANES), F32),
        ),
        in_specs=[hbm] * 6,
        out_specs=(hbm, hbm, vmem),
        scratch_shapes=[
            pltpu.VMEM((ext, nz, ny), F32),
            pltpu.VMEM((ext, nz, ny), jnp.int32),
            pltpu.VMEM((2, STEPS, 2, rows_x, GROUP, LANES), BF),
            pltpu.VMEM((STEPS, 2, rows_x, GROUP, LANES), BF),
            pltpu.VMEM((index.shape[1], 8), F32),
            pltpu.VMEM((units // LANES, 8, LANES), F32),
            pltpu.VMEM((n_run - 1, 8, LANES), F32),
            pltpu.VMEM((8, LANES), F32),
            pltpu.VMEM((n_strip - 1, 8, LANES), F32),
            dma((2,)), dma((4,)), dma((4,)), dma((4,)), dma((STEPS, 2)), dma((STEPS, 2)),
            dma((blocks,)), dma((blocks,)),
            dma((n_run - 1,)), dma((n_run - 1,)), dma((n_strip - 1,)), dma((n_strip - 1,)),
        ],
        compiler_params=pltpu.CompilerParams(
            collective_id=0, has_side_effects=True, vmem_limit_bytes=63 * 1024 * 1024
        ),
        name="forward",
    )(levels, index, w_in, base, material, weight)


def output_kernel(hid_in, total, error, grad, turned, hid, e_all, g_all, h_sem, e_sem, g_sem):
    blocks = e_all.shape[0]
    fetches = [pltpu.make_async_copy(error.at[i], e_all.at[i], e_sem.at[i]) for i in range(blocks)]
    first = pltpu.make_async_copy(hid_in, hid, h_sem)
    for copy in [first] + fetches:
        copy.start()
    turned[...] = total[...].T[: turned.shape[0]]
    puts = []
    first.wait()
    for i in range(blocks):
        fetches[i].wait()
        g = jnp.dot(hid[...], e_all[i], preferred_element_type=F32).astype(BF)
        g = jnp.stack([g[:, x * LANES : (x + 1) * LANES] for x in range(WIDTH)], axis=0)
        g_all[i] = jnp.swapaxes(g, 0, 1)
        puts.append(
            pltpu.make_async_copy(
                g_all.at[i], grad.at[:, pl.ds(i * WIDTH, WIDTH), :], g_sem.at[i]
            )
        )
        puts[-1].start()
    for copy in puts:
        copy.wait()


def output_gradient(hid, total, error, keep):
    units, batch = hid.shape
    blocks = error.shape[0]
    hbm = pl.BlockSpec(memory_space=pl.ANY)
    vmem = pl.BlockSpec(memory_space=pltpu.VMEM)
    return pl.pallas_call(
        output_kernel,
        out_shape=(
            jax.ShapeDtypeStruct((units, blocks * WIDTH, LANES), BF),
            jax.ShapeDtypeStruct((keep, 8), F32),
        ),
        in_specs=[hbm, vmem, hbm],
        out_specs=(hbm, vmem),
        scratch_shapes=[
            pltpu.VMEM(hid.shape, BF),
            pltpu.VMEM(error.shape, BF),
            pltpu.VMEM((blocks, units, WIDTH, LANES), BF),
            pltpu.SemaphoreType.DMA,
            pltpu.SemaphoreType.DMA((blocks,)),
            pltpu.SemaphoreType.DMA((blocks,)),
        ],
        compiler_params=pltpu.CompilerParams(vmem_limit_bytes=63 * 1024 * 1024),
        name="output_gradient",
    )(hid, total, error)


def solution(mesh):
    n_run, n_strip = mesh.shape["run"], mesh.shape["strip"]

    def local(base_field, material_map, param_levels, param_index, w_input, w_output):
        error, hid, total = forward(
            param_levels, param_index.T, w_input, base_field, material_map, w_output, n_run, n_strip
        )
        keep = w_output.shape[0] // (n_run * n_strip)
        grad_output, turned = output_gradient(hid, total, error, keep)
        return grad_output, turned.T

    placed = (
        P("strip", None, None),
        P("strip", None, None),
        P(),
        P(),
        P(),
        P(None, "strip", "run"),
    )
    return jax.shard_map(
        local,
        mesh=mesh,
        in_specs=placed,
        out_specs=(P(None, "strip", "run"), P(None, ("run", "strip"))),
        check_vma=False,
    )
```

```python
import functools

import jax
import jax.numpy as jnp
from jax import lax
from jax.experimental import pallas as pl
from jax.experimental.pallas import tpu as pltpu
from jax.sharding import PartitionSpec as P

STEPS = 4
TIME_STEP = 0.08
BF = jnp.bfloat16
F32 = jnp.float32
MESH = pl.DeviceIdType.MESH
GROUP = 16
LANES = 128
CHUNK = 35
WIDTH = 8
TURN = 2


def run_values(levels_ref, index_ref):
    rows = []
    for p in range(index_ref.shape[0]):
        row = index_ref[p : p + 1, :]
        out = jnp.zeros(row.shape, F32)
        for level in range(levels_ref.shape[1]):
            out = jnp.where(row == level, levels_ref[p : p + 1, level : level + 1], out)
        rows.append(out)
    rows.append(jnp.zeros((8 - len(rows), index_ref.shape[1]), F32))
    return jnp.concatenate(rows, axis=0).T


def forward_kernel(n_run, n_strip, levels_in, index_in, w_in_in, base, material, weight, *rest):
    rows_x, nz, _ = base.shape
    units = weight.shape[0]
    batch = STEPS * index_in.shape[1]
    blocks = rows_x // WIDTH
    ext = rows_x + 2 * STEPS
    field = pltpu.VMEM((nz + 2, ext, 2, GROUP, LANES), BF)
    inner = pltpu.VMEM((nz, ext, 2, GROUP, LANES), BF)
    row = pltpu.VMEM((ext, 2, GROUP, LANES), BF)
    pl.run_scoped(
        functools.partial(
            forward_body, n_run, n_strip, levels_in, index_in, w_in_in, base, material, weight, *rest
        ),
        field, field, field, field, inner, inner, row, row, row,
        pltpu.VMEM((2, 2 * LANES, 2 * LANES), BF),
        pltpu.VMEM((blocks, units, WIDTH, LANES), BF),
        pltpu.VMEM((blocks, batch, WIDTH * LANES), BF),
        pltpu.VMEM((index_in.shape[1], units), F32),
        pltpu.VMEM((batch, units), F32),
        pltpu.VMEM((batch, units), BF),
        pltpu.VMEM((units, batch), BF),
        pltpu.VMEM((batch, units), F32),
        pltpu.VMEM(levels_in.shape, F32),
        pltpu.VMEM(index_in.shape, jnp.int32),
        pltpu.VMEM(w_in_in.shape, F32),
    )


def forward_body(
    n_run, n_strip, levels_in, index_in, w_in_in, base, material, weight,
    error_out, hid_out, grad_out,
    bx, mx, shots, landed, values, partial, got_run, mid, got_strip,
    local_sem, small_sem, halo_send, halo_recv, send_sem, recv_sem, w_sem, e_sem,
    s_run, r_run, s_strip, r_strip,
    u_a, u_b, k_a, k_b, cond, cond_g, tops, flux_y, flux_next, shifts,
    w_all, e_all, mixed, hid, hid_b, hid_t, back, levels, index, w_in,
):
    rows_x, nz, ny = base.shape
    ext = rows_x + 2 * STEPS
    run = lax.axis_index("run")
    strip = lax.axis_index("strip")
    core = lax.rem(run, 2)
    slab = lax.div(run, 2)
    partner = run + 1 - 2 * core
    right = lax.rem(strip + 1, n_strip)
    left = lax.rem(strip + n_strip - 1, n_strip)

    local = [
        pltpu.make_async_copy(src, dst.at[pl.ds(STEPS, rows_x)], local_sem.at[i])
        for i, (src, dst) in enumerate(((base, bx), (material, mx)))
    ]
    small = [
        pltpu.make_async_copy(src, dst, small_sem.at[i])
        for i, (src, dst) in enumerate(((levels_in, levels), (index_in, index), (w_in_in, w_in)))
    ]
    for copy in small + local:
        copy.start()
    blocks = rows_x // WIDTH
    fetches = [
        pltpu.make_async_copy(
            weight.at[:, pl.ds(i * WIDTH, WIDTH), :], w_all.at[i], w_sem.at[i]
        )
        for i in range(blocks)
    ]
    barrier = pltpu.get_barrier_semaphore()
    peers = [{"run": lax.rem(run + j, n_run)} for j in range(1, n_run)]
    peers += [{"strip": lax.rem(strip + j, n_strip)} for j in range(1, n_strip)]
    for where in peers:
        pl.semaphore_signal(barrier, inc=1, device_id=where, device_id_type=MESH)
    halos = []
    for i, dst in enumerate((bx, mx)):
        for j, (first, to, target) in enumerate(
            ((rows_x, 0, right), (STEPS, STEPS + rows_x, left))
        ):
            halos.append(
                pltpu.make_async_remote_copy(
                    src_ref=dst.at[pl.ds(first, STEPS)],
                    dst_ref=dst.at[pl.ds(to, STEPS)],
                    send_sem=halo_send.at[2 * i + j],
                    recv_sem=halo_recv.at[2 * i + j],
                    device_id={"strip": target},
                    device_id_type=MESH,
                )
            )
    hid_put = pltpu.make_async_copy(hid_t, hid_out, small_sem.at[3])
    zero_row = jnp.zeros((2, GROUP, LANES), BF)

    def clear(pad):
        def body(x, carry):
            for ref in (u_a, u_b, k_a, k_b):
                ref[pad, x] = zero_row
            return carry

        lax.fori_loop(0, ext, body, 0)

    clear(0)
    clear(nz + 1)
    for copy in small:
        copy.wait()
    for copy in fetches:
        copy.start()
    vals = run_values(levels, index)
    values[...] = vals

    lane = lax.broadcasted_iota(jnp.int32, (GROUP, LANES), 1).astype(F32).astype(BF)
    first_lane = lane == jnp.asarray(0, BF)
    way = jnp.where(slab >= nz // 2, -1, 1)
    down = lax.broadcasted_iota(jnp.int32, (ny, ny), 0)
    across = lax.broadcasted_iota(jnp.int32, (ny, ny), 1)
    after = (down == across + 1).astype(F32)
    same = (down == across).astype(F32)
    shifts[0] = (after - same).astype(BF)
    shifts[1] = (after + same).astype(BF)

    def prepare(g):
        mine = values[pl.ds(pl.multiple_of(core * 2 * GROUP + g * GROUP, GROUP), GROUP), :]
        vals = [mine[:, p : p + 1] for p in range(6)]
        wide = lambda col: jnp.broadcast_to(col, (GROUP, LANES))
        kinds = [wide(0.5 * TIME_STEP * vals[m]).astype(BF) for m in range(4)]
        growth = wide(0.1 * vals[4]).astype(BF)
        start = wide(vals[5])
        return kinds, growth, start

    def fill(first, count, unroll, kinds, growth, start):
        def one(x):
            tile = bx[x]
            mats = mx[x].astype(F32)
            for z in range(nz):
                for h in range(2):
                    cut = slice(h * LANES, (h + 1) * LANES)
                    mat = jnp.broadcast_to(mats[z : z + 1, cut], (GROUP, LANES)).astype(BF)
                    c = kinds[0]
                    for m in range(1, 4):
                        c = jnp.where(mat == jnp.asarray(m, BF), kinds[m], c)
                    cg = c * growth
                    u = (jnp.broadcast_to(tile[z : z + 1, cut], (GROUP, LANES)) * start).astype(BF)
                    cond[z, x, h] = c
                    cond_g[z, x, h] = cg
                    u_a[z + 1, x, h] = u
                    k_a[z + 1, x, h] = c + cg * (u * u)

        def body(i, carry):
            for j in range(unroll):
                one(first + i * unroll + j)
            return carry

        lax.fori_loop(0, count // unroll, body, 0)

    def blank(refs, first, count):
        def body(z, carry):
            for x in range(first, first + count):
                for ref, shift in refs:
                    ref[z + shift, x] = zero_row
            return carry

        lax.fori_loop(0, nz, body, 0)

    def halves(ref, a, x):
        return [ref[a, x, 0], ref[a, x, 1]]

    def flat(block):
        count = block.shape[0] * GROUP
        sides = [block[:, h].reshape(count, LANES) for h in range(2)]
        return jnp.concatenate(sides, axis=1)

    def along_y(us, ks, zp, first, count):
        u, k = us[zp, pl.ds(first, count)], ks[zp, pl.ds(first, count)]
        rise = jnp.dot(flat(u), shifts[0], preferred_element_type=F32).astype(BF)
        pair = jnp.dot(flat(k), shifts[1], preferred_element_type=F32).astype(BF)
        face = rise * pair
        out = []
        for j in range(count):
            f = [face[j * GROUP : (j + 1) * GROUP, h * LANES : (h + 1) * LANES] for h in range(2)]
            r = [pltpu.roll(v, 1, 1) for v in f]
            out.append(
                [
                    f[0] - jnp.where(first_lane, k[j, 0] * u[j, 0], r[0]),
                    f[1] - jnp.where(first_lane, r[0], r[1]),
                ]
            )
        return out

    def keep_y(flux, first, ref):
        for j, pair in enumerate(flux):
            for h in range(2):
                ref[first + j, h] = pair[h]

    def pieces(step, part):
        if part == "inner":
            return [(STEPS + step, rows_x - 2 * step)]
        if part == "edge":
            return [(step, STEPS), (ext - step - STEPS, STEPS)]
        return [(step, ext - 2 * step)]

    def chunks(step, part):
        return [
            (x, min(CHUNK, first + count - x), x == first)
            for first, count in pieces(step, part)
            for x in range(first, first + count, CHUNK)
        ]

    def span(step):
        reach = STEPS - step
        low = jnp.maximum(slab - reach, 0)
        high = jnp.minimum(slab + reach, nz - 1)
        return jnp.where(way > 0, low, high), high - low + 1

    def start_y(us, ks, part):
        zp = span(1)[0] + 1
        for first, count, _ in chunks(1, part):
            keep_y(along_y(us, ks, zp, first, count), first, flux_y)

    def advance(step, g, us, ks, ud, kd, part):
        final = step == STEPS
        begin, number = span(step)

        def one_slab(z, last):
            zp = z + 1
            after = (span(step + 1)[0] + 1) if last else zp + way
            src = (ud, kd) if last else (us, ks)
            if last and not final:
                for first, count, _ in chunks(step + 1, part):
                    keep_y(along_y(*src, after, first, count), first, flux_next)
            for first, count, fresh in chunks(step, part):
                if fresh:
                    u, k = halves(us, zp, first), halves(ks, zp, first)
                    ub, kb = halves(us, zp, first - 1), halves(ks, zp, first - 1)
                    fl = [(k[h] + kb[h]) * (u[h] - ub[h]) for h in range(2)]
                flux = None if last else along_y(*src, after, first, count)
                for x in range(first, first + count):
                    un, kn = halves(us, zp, x + 1), halves(ks, zp, x + 1)
                    uz, kz = halves(us, zp + way, x), halves(ks, zp + way, x)
                    fr = []
                    for h in range(2):
                        face = (k[h] + kn[h]) * (un[h] - u[h])
                        top = (k[h] + kz[h]) * (uz[h] - u[h])
                        total = (face - fl[h]) + (top - tops[x, h]) + flux_y[x, h]
                        new = u[h] + total
                        if final:
                            shots[h, step - 1, g, x - STEPS] = new
                        else:
                            if not last:
                                tops[x, h] = top
                            ud[zp, x, h] = new
                            kd[zp, x, h] = cond[z, x, h] + cond_g[z, x, h] * (new * new)
                        fr.append(face)
                    u, k, fl = un, kn, fr
                if flux is not None:
                    keep_y(flux, first, flux_y)
            if last and not final:
                for first, count in pieces(step + 1, part):
                    for x in range(first, first + count):
                        for h in range(2):
                            flux_y[x, h] = flux_next[x, h]

        def first_faces(first, i, carry):
            for j in range(2):
                x = first + i * 2 + j
                for h in range(2):
                    du = us[begin + 1, x, h] - us[begin + 1 - way, x, h]
                    tops[x, h] = (ks[begin + 1, x, h] + ks[begin + 1 - way, x, h]) * du
            return carry

        def slabs(i, carry):
            one_slab(begin + way * i, False)
            return carry

        for first, count in pieces(step, part):
            lax.fori_loop(0, count // 2, functools.partial(first_faces, first), 0)
        if not final:
            lax.fori_loop(0, number - 1, slabs, 0)
        one_slab(begin + way * (number - 1), True)
        if final:
            return
        if part != "inner":

            @pl.when(strip == 0)
            def _():
                blank([(ud, 1)], 0, STEPS)

            @pl.when(strip == n_strip - 1)
            def _():
                blank([(ud, 1)], STEPS + rows_x, STEPS)

        def keep(x):
            for h in range(2):
                shots[h, step - 1, g, x - STEPS] = ud[slab + 1, x, h]

        if part == "edge":
            for j in range(step):
                keep(STEPS + j)
                keep(STEPS + rows_x - 1 - j)
            return
        first, count = (STEPS, rows_x) if part == "full" else pieces(step, part)[0]

        def several_rows(i, carry):
            for j in range(2):
                keep(first + i * 2 + j)
            return carry

        lax.fori_loop(0, count // 2, several_rows, 0)

    def send(step, g):
        return pltpu.make_async_remote_copy(
            src_ref=shots.at[1 - core, step - 1, g],
            dst_ref=landed.at[step - 1, g],
            send_sem=send_sem.at[step - 1, g],
            recv_sem=recv_sem.at[step - 1, g],
            device_id={"run": partner},
            device_id_type=MESH,
        )

    fields = [(u_a, k_a), (u_b, k_b)]
    everywhere = [(cond, 0), (cond_g, 0), (u_a, 1), (k_a, 1)]

    def all_edges():
        @pl.when(strip == 0)
        def _():
            blank(everywhere, 0, STEPS)

        @pl.when(strip == n_strip - 1)
        def _():
            blank(everywhere, STEPS + rows_x, STEPS)

    def move(step, g, part):
        advance(step, g, *fields[(step - 1) % 2], *fields[step % 2], part)

    consts = prepare(0)
    for copy in local:
        copy.wait()
    fill(STEPS, rows_x, 2, *consts)
    hidden_layer(vals, w_in, core, mixed, hid, hid_b, hid_t)
    hid_put.start()

    def group(g, carry):
        @pl.when(g > 0)
        def _():
            fill(0, ext, 2, *prepare(g))

        start_y(u_a, k_a, "inner")
        move(1, g, "inner")

        @pl.when(g == 0)
        def _():
            pl.semaphore_wait(barrier, n_run + n_strip - 2)
            for copy in halos:
                copy.start()

        for step in range(2, STEPS + 1):
            move(step, g, "inner")

        @pl.when(g == 0)
        def _():
            for copy in halos:
                copy.wait()
            fill(0, STEPS, 1, *prepare(g))
            fill(STEPS + rows_x, STEPS, 1, *prepare(g))

        all_edges()
        start_y(u_a, k_a, "edge")
        for step in range(1, STEPS + 1):
            move(step, g, "edge")
            send(step, g).start()
        return carry

    lax.fori_loop(0, 2, group, 0)
    for copy in fetches:
        copy.wait()
    back[...] = jnp.zeros_like(back)
    for g in range(2):
        for step in range(1, STEPS + 1):
            send(step, g).wait()

    batch = hid.shape[0]

    def put(i):
        return pltpu.make_async_copy(e_all.at[i], error_out.at[i], e_sem.at[i])

    def train(i):
        w = jnp.swapaxes(w_all[i], 0, 1)
        w = jnp.concatenate([w[x] for x in range(WIDTH)], axis=1)
        pred = jnp.dot(hid_b[...], w, preferred_element_type=F32)
        cuts = []
        for x in range(WIDTH):
            at = i * WIDTH + x
            tiles = [shots[core, t, g, at] for t in range(STEPS) for g in range(2)]
            tiles += [landed[t, g, at] for t in range(STEPS) for g in range(2)]
            cuts.append(jnp.concatenate(tiles, axis=0))
        goal = jnp.concatenate(cuts, axis=1)
        error = ((pred - goal.astype(F32)) * (batch ** -0.5)).astype(BF)
        e_all[i] = error
        put(i).start()
        return lax.dot_general(error, w, (((1,), (1,)), ((), ())), preferred_element_type=F32)

    def several(i, carry):
        back[...] += sum(train(i * TURN + j) for j in range(TURN))
        return carry

    lax.fori_loop(0, blocks // TURN, several, 0)
    input_gradient(values, core, hid, back, partial)
    reduce_scatter(
        n_run, n_strip, partial, grad_out, got_run, mid, got_strip, s_run, r_run, s_strip, r_strip
    )
    hid_put.wait()
    for i in range(blocks):
        put(i).wait()


def hidden_layer(vals, w_in, core, mixed, hid, hid_b, hid_t):
    half = 2 * GROUP
    total = vals[:, 0:1] * w_in[0:1, :]
    for p in range(1, 6):
        total = total + vals[:, p : p + 1] * w_in[p : p + 1, :]
    mixed[...] = total
    for part in range(2):
        owner = core if part == 0 else 1 - core
        rows = mixed[pl.ds(pl.multiple_of(owner * half, half), half), :]
        for t in range(STEPS):
            pre = rows + ((t + 1.0) / STEPS) * w_in[6:7, :] + w_in[7:8, :]
            hid[pl.ds((part * STEPS + t) * half, half), :] = jnp.tanh(pre)
    hid_b[...] = hid[...].astype(BF)
    hid_t[...] = hid[...].T.astype(BF)


def input_gradient(values, core, hid, back, partial):
    half = 2 * GROUP
    h = hid[...]
    slope = back[...] * (1.0 - h * h)
    steps = [
        [slope[(part * STEPS + t) * half : (part * STEPS + t + 1) * half] for t in range(STEPS)]
        for part in range(2)
    ]
    runs = [p[0] + p[1] + p[2] + p[3] for p in steps]
    vals = [
        values[pl.ds(pl.multiple_of((core if part == 0 else 1 - core) * half, half), half), :]
        for part in range(2)
    ]
    rows = []
    for p in range(6):
        both = vals[0][:, p : p + 1] * runs[0] + vals[1][:, p : p + 1] * runs[1]
        rows.append(jnp.sum(both, axis=0, keepdims=True))
    timed = sum(((t + 1.0) / STEPS) * (steps[0][t] + steps[1][t]) for t in range(STEPS))
    rows.append(jnp.sum(timed, axis=0, keepdims=True))
    rows.append(jnp.sum(runs[0] + runs[1], axis=0, keepdims=True))
    full = jnp.concatenate(rows, axis=0)
    for q in range(partial.shape[0]):
        partial[q] = full[:, q * LANES : (q + 1) * LANES]


def reduce_scatter(
    n_run, n_strip, partial, out, got_run, mid, got_strip, s_run, r_run, s_strip, r_strip
):
    run = lax.axis_index("run")
    strip = lax.axis_index("strip")
    units = partial.shape[0] * LANES
    keep = units // (n_run * n_strip)
    per = LANES // (n_strip * keep)
    copies = []
    for j in range(1, n_run):
        to = lax.rem(run + j, n_run)
        copies.append(
            pltpu.make_async_remote_copy(
                src_ref=partial.at[lax.div(to, per)],
                dst_ref=got_run.at[j - 1],
                send_sem=s_run.at[j - 1],
                recv_sem=r_run.at[j - 1],
                device_id={"run": to},
                device_id_type=MESH,
            )
        )
        copies[-1].start()
    total = partial[lax.div(run, per)]
    for j in range(n_run - 1):
        copies[j].wait_recv()
        total = total + got_run[j]
    mid[...] = total
    more = []
    for j in range(1, n_strip):
        to = lax.rem(strip + j, n_strip)
        more.append(
            pltpu.make_async_remote_copy(
                src_ref=mid,
                dst_ref=got_strip.at[j - 1],
                send_sem=s_strip.at[j - 1],
                recv_sem=r_strip.at[j - 1],
                device_id={"strip": to},
                device_id_type=MESH,
            )
        )
        more[-1].start()
    for j in range(n_strip - 1):
        more[j].wait_recv()
        total = total + got_strip[j]
    for copy in copies + more:
        copy.wait_send()
    at = lax.rem(run, per) * (n_strip * keep) + strip * keep
    out[...] = pltpu.roll(total, lax.rem(LANES - at, LANES), 1)


def forward(levels, index, w_in, base, material, weight, n_run, n_strip):
    rows_x, nz, ny = base.shape
    units = weight.shape[0]
    batch = STEPS * index.shape[1]
    blocks = rows_x // WIDTH
    ext = rows_x + 2 * STEPS
    hbm = pl.BlockSpec(memory_space=pl.ANY)
    vmem = pl.BlockSpec(memory_space=pltpu.VMEM)
    dma = pltpu.SemaphoreType.DMA
    return pl.pallas_call(
        functools.partial(forward_kernel, n_run, n_strip),
        out_shape=(
            jax.ShapeDtypeStruct((blocks, batch, WIDTH * LANES), BF),
            jax.ShapeDtypeStruct((units, batch), BF),
            jax.ShapeDtypeStruct((8, LANES), F32),
        ),
        in_specs=[hbm] * 6,
        out_specs=(hbm, hbm, vmem),
        scratch_shapes=[
            pltpu.VMEM((ext, nz, ny), F32),
            pltpu.VMEM((ext, nz, ny), jnp.int32),
            pltpu.VMEM((2, STEPS, 2, rows_x, GROUP, LANES), BF),
            pltpu.VMEM((STEPS, 2, rows_x, GROUP, LANES), BF),
            pltpu.VMEM((index.shape[1], 8), F32),
            pltpu.VMEM((units // LANES, 8, LANES), F32),
            pltpu.VMEM((n_run - 1, 8, LANES), F32),
            pltpu.VMEM((8, LANES), F32),
            pltpu.VMEM((n_strip - 1, 8, LANES), F32),
            dma((2,)), dma((4,)), dma((4,)), dma((4,)), dma((STEPS, 2)), dma((STEPS, 2)),
            dma((blocks,)), dma((blocks,)),
            dma((n_run - 1,)), dma((n_run - 1,)), dma((n_strip - 1,)), dma((n_strip - 1,)),
        ],
        compiler_params=pltpu.CompilerParams(
            collective_id=0, has_side_effects=True, vmem_limit_bytes=63 * 1024 * 1024
        ),
        name="forward",
    )(levels, index, w_in, base, material, weight)


def output_kernel(hid, total, error, grad, turned, e_all, g_all, e_sem, g_sem):
    blocks = e_all.shape[0]
    fetches = [pltpu.make_async_copy(error.at[i], e_all.at[i], e_sem.at[i]) for i in range(blocks)]
    for copy in fetches:
        copy.start()
    turned[...] = total[...].T[: turned.shape[0]]
    puts = []
    for i in range(blocks):
        fetches[i].wait()
        g = jnp.dot(hid[...], e_all[i], preferred_element_type=F32).astype(BF)
        g = jnp.stack([g[:, x * LANES : (x + 1) * LANES] for x in range(WIDTH)], axis=0)
        g_all[i] = jnp.swapaxes(g, 0, 1)
        puts.append(
            pltpu.make_async_copy(
                g_all.at[i], grad.at[:, pl.ds(i * WIDTH, WIDTH), :], g_sem.at[i]
            )
        )
        puts[-1].start()
    for copy in puts:
        copy.wait()


def output_gradient(hid, total, error, keep):
    units, batch = hid.shape
    blocks = error.shape[0]
    hbm = pl.BlockSpec(memory_space=pl.ANY)
    vmem = pl.BlockSpec(memory_space=pltpu.VMEM)
    return pl.pallas_call(
        output_kernel,
        out_shape=(
            jax.ShapeDtypeStruct((units, blocks * WIDTH, LANES), BF),
            jax.ShapeDtypeStruct((keep, 8), F32),
        ),
        in_specs=[vmem, vmem, hbm],
        out_specs=(hbm, vmem),
        scratch_shapes=[
            pltpu.VMEM(error.shape, BF),
            pltpu.VMEM((blocks, units, WIDTH, LANES), BF),
            pltpu.SemaphoreType.DMA((blocks,)),
            pltpu.SemaphoreType.DMA((blocks,)),
        ],
        compiler_params=pltpu.CompilerParams(vmem_limit_bytes=63 * 1024 * 1024),
        name="output_gradient",
    )(hid, total, error)


def solution(mesh):
    n_run, n_strip = mesh.shape["run"], mesh.shape["strip"]

    def local(base_field, material_map, param_levels, param_index, w_input, w_output):
        error, hid, total = forward(
            param_levels, param_index.T, w_input, base_field, material_map, w_output, n_run, n_strip
        )
        keep = w_output.shape[0] // (n_run * n_strip)
        grad_output, turned = output_gradient(hid, total, error, keep)
        return grad_output, turned.T

    placed = (
        P("strip", None, None),
        P("strip", None, None),
        P(),
        P(),
        P(),
        P(None, "strip", "run"),
    )
    return jax.shard_map(
        local,
        mesh=mesh,
        in_specs=placed,
        out_specs=(P(None, "strip", "run"), P(None, ("run", "strip"))),
        check_vma=False,
    )
```

```python
import functools

import jax
import jax.numpy as jnp
from jax import lax
from jax.experimental import pallas as pl
from jax.experimental.pallas import tpu as pltpu
from jax.sharding import PartitionSpec as P

STEPS = 4
TIME_STEP = 0.08
BF = jnp.bfloat16
F32 = jnp.float32
MESH = pl.DeviceIdType.MESH
GROUP = 16
LANES = 128
CHUNK = 35
WIDTH = 8
TURN = 2
AHEAD = 3


def run_values(levels_ref, index_ref):
    rows = []
    for p in range(index_ref.shape[0]):
        row = index_ref[p : p + 1, :]
        out = jnp.zeros(row.shape, F32)
        for level in range(levels_ref.shape[1]):
            out = jnp.where(row == level, levels_ref[p : p + 1, level : level + 1], out)
        rows.append(out)
    rows.append(jnp.zeros((8 - len(rows), index_ref.shape[1]), F32))
    return jnp.concatenate(rows, axis=0).T


def forward_kernel(n_run, n_strip, levels_in, index_in, w_in_in, base, material, weight, *rest):
    rows_x, nz, _ = base.shape
    units = weight.shape[0]
    batch = STEPS * index_in.shape[1]
    blocks = rows_x // WIDTH
    ext = rows_x + 2 * STEPS
    field = pltpu.VMEM((nz + 2, ext, 2, GROUP, LANES), BF)
    inner = pltpu.VMEM((nz, ext, 2, GROUP, LANES), BF)
    row = pltpu.VMEM((ext, 2, GROUP, LANES), BF)
    pl.run_scoped(
        functools.partial(
            forward_body, n_run, n_strip, levels_in, index_in, w_in_in, base, material, weight, *rest
        ),
        field, field, field, field, inner, inner, row, row, row,
        pltpu.VMEM((2, 2 * LANES, 2 * LANES), BF),
        pltpu.VMEM((blocks, units, WIDTH, LANES), BF),
        pltpu.VMEM((blocks, batch, WIDTH * LANES), BF),
        pltpu.VMEM((index_in.shape[1], units), F32),
        pltpu.VMEM((batch, units), F32),
        pltpu.VMEM((batch, units), BF),
        pltpu.VMEM((units, batch), BF),
        pltpu.VMEM((batch, units), F32),
        pltpu.VMEM(levels_in.shape, F32),
        pltpu.VMEM(index_in.shape, jnp.int32),
        pltpu.VMEM(w_in_in.shape, F32),
    )


def forward_body(
    n_run, n_strip, levels_in, index_in, w_in_in, base, material, weight,
    error_out, hid_out, grad_out,
    bx, mx, shots, landed, values, partial, got_run, mid, got_strip,
    local_sem, small_sem, halo_send, halo_recv, send_sem, recv_sem, w_sem, e_sem,
    s_run, r_run, s_strip, r_strip,
    u_a, u_b, k_a, k_b, cond, cond_g, tops, flux_y, flux_next, shifts,
    w_all, e_all, mixed, hid, hid_b, hid_t, back, levels, index, w_in,
):
    rows_x, nz, ny = base.shape
    ext = rows_x + 2 * STEPS
    run = lax.axis_index("run")
    strip = lax.axis_index("strip")
    core = lax.rem(run, 2)
    slab = lax.div(run, 2)
    partner = run + 1 - 2 * core
    right = lax.rem(strip + 1, n_strip)
    left = lax.rem(strip + n_strip - 1, n_strip)

    local = [
        pltpu.make_async_copy(src, dst.at[pl.ds(STEPS, rows_x)], local_sem.at[i])
        for i, (src, dst) in enumerate(((base, bx), (material, mx)))
    ]
    small = [
        pltpu.make_async_copy(src, dst, small_sem.at[i])
        for i, (src, dst) in enumerate(((levels_in, levels), (index_in, index), (w_in_in, w_in)))
    ]
    for copy in small + local:
        copy.start()
    blocks = rows_x // WIDTH
    fetches = [
        pltpu.make_async_copy(
            weight.at[:, pl.ds(i * WIDTH, WIDTH), :], w_all.at[i], w_sem.at[i]
        )
        for i in range(blocks)
    ]
    barrier = pltpu.get_barrier_semaphore()
    peers = [{"run": lax.rem(run + j, n_run)} for j in range(1, n_run)]
    peers += [{"strip": lax.rem(strip + j, n_strip)} for j in range(1, n_strip)]
    for where in peers:
        pl.semaphore_signal(barrier, inc=1, device_id=where, device_id_type=MESH)
    halos = []
    for i, dst in enumerate((bx, mx)):
        for j, (first, to, target) in enumerate(
            ((rows_x, 0, right), (STEPS, STEPS + rows_x, left))
        ):
            halos.append(
                pltpu.make_async_remote_copy(
                    src_ref=dst.at[pl.ds(first, STEPS)],
                    dst_ref=dst.at[pl.ds(to, STEPS)],
                    send_sem=halo_send.at[2 * i + j],
                    recv_sem=halo_recv.at[2 * i + j],
                    device_id={"strip": target},
                    device_id_type=MESH,
                )
            )
    hid_put = pltpu.make_async_copy(hid_t, hid_out, small_sem.at[3])
    zero_row = jnp.zeros((2, GROUP, LANES), BF)

    def clear(pad):
        def body(x, carry):
            for ref in (u_a, u_b, k_a, k_b):
                ref[pad, x] = zero_row
            return carry

        lax.fori_loop(0, ext, body, 0)

    clear(0)
    clear(nz + 1)
    for copy in small:
        copy.wait()
    vals = run_values(levels, index)
    values[...] = vals

    lane = lax.broadcasted_iota(jnp.int32, (GROUP, LANES), 1).astype(F32).astype(BF)
    first_lane = lane == jnp.asarray(0, BF)
    way = jnp.where(slab >= nz // 2, -1, 1)
    down = lax.broadcasted_iota(jnp.int32, (ny, ny), 0)
    across = lax.broadcasted_iota(jnp.int32, (ny, ny), 1)
    after = (down == across + 1).astype(F32)
    same = (down == across).astype(F32)
    shifts[0] = (after - same).astype(BF)
    shifts[1] = (after + same).astype(BF)

    def prepare(g):
        mine = values[pl.ds(pl.multiple_of(core * 2 * GROUP + g * GROUP, GROUP), GROUP), :]
        vals = [mine[:, p : p + 1] for p in range(6)]
        wide = lambda col: jnp.broadcast_to(col, (GROUP, LANES))
        kinds = [wide(0.5 * TIME_STEP * vals[m]).astype(BF) for m in range(4)]
        growth = wide(0.1 * vals[4]).astype(BF)
        start = wide(vals[5])
        return kinds, growth, start

    def fill(first, count, unroll, kinds, growth, start):
        def one(x):
            tile = bx[x]
            mats = mx[x].astype(F32)
            for z in range(nz):
                for h in range(2):
                    cut = slice(h * LANES, (h + 1) * LANES)
                    mat = jnp.broadcast_to(mats[z : z + 1, cut], (GROUP, LANES)).astype(BF)
                    c = kinds[0]
                    for m in range(1, 4):
                        c = jnp.where(mat == jnp.asarray(m, BF), kinds[m], c)
                    cg = c * growth
                    u = (jnp.broadcast_to(tile[z : z + 1, cut], (GROUP, LANES)) * start).astype(BF)
                    cond[z, x, h] = c
                    cond_g[z, x, h] = cg
                    u_a[z + 1, x, h] = u
                    k_a[z + 1, x, h] = c + cg * (u * u)

        def body(i, carry):
            for j in range(unroll):
                one(first + i * unroll + j)
            return carry

        lax.fori_loop(0, count // unroll, body, 0)

    def blank(refs, first, count):
        def body(z, carry):
            for x in range(first, first + count):
                for ref, shift in refs:
                    ref[z + shift, x] = zero_row
            return carry

        lax.fori_loop(0, nz, body, 0)

    def halves(ref, a, x):
        return [ref[a, x, 0], ref[a, x, 1]]

    def flat(block):
        count = block.shape[0] * GROUP
        sides = [block[:, h].reshape(count, LANES) for h in range(2)]
        return jnp.concatenate(sides, axis=1)

    def along_y(us, ks, zp, first, count):
        u, k = us[zp, pl.ds(first, count)], ks[zp, pl.ds(first, count)]
        rise = jnp.dot(flat(u), shifts[0], preferred_element_type=F32).astype(BF)
        pair = jnp.dot(flat(k), shifts[1], preferred_element_type=F32).astype(BF)
        face = rise * pair
        out = []
        for j in range(count):
            f = [face[j * GROUP : (j + 1) * GROUP, h * LANES : (h + 1) * LANES] for h in range(2)]
            r = [pltpu.roll(v, 1, 1) for v in f]
            out.append(
                [
                    f[0] - jnp.where(first_lane, k[j, 0] * u[j, 0], r[0]),
                    f[1] - jnp.where(first_lane, r[0], r[1]),
                ]
            )
        return out

    def keep_y(flux, first, ref):
        for j, pair in enumerate(flux):
            for h in range(2):
                ref[first + j, h] = pair[h]

    def chunks(step):
        return [(x, min(CHUNK, ext - step - x)) for x in range(step, ext - step, CHUNK)]

    def span(step):
        reach = STEPS - step
        low = jnp.maximum(slab - reach, 0)
        high = jnp.minimum(slab + reach, nz - 1)
        return jnp.where(way > 0, low, high), high - low + 1

    def start_y(us, ks):
        zp = span(1)[0] + 1
        for first, count in chunks(1):
            keep_y(along_y(us, ks, zp, first, count), first, flux_y)

    def advance(step, g, us, ks, ud, kd):
        final = step == STEPS
        begin, number = span(step)

        def one_slab(z, last):
            zp = z + 1
            after = (span(step + 1)[0] + 1) if last else zp + way
            src = (ud, kd) if last else (us, ks)
            if last and not final:
                for first, count in chunks(step):
                    keep_y(along_y(*src, after, first, count), first, flux_next)
            u, k = halves(us, zp, step), halves(ks, zp, step)
            ub, kb = halves(us, zp, step - 1), halves(ks, zp, step - 1)
            fl = [(k[h] + kb[h]) * (u[h] - ub[h]) for h in range(2)]
            for first, count in chunks(step):
                flux = None if last else along_y(*src, after, first, count)
                for x in range(first, first + count):
                    un, kn = halves(us, zp, x + 1), halves(ks, zp, x + 1)
                    uz, kz = halves(us, zp + way, x), halves(ks, zp + way, x)
                    fr = []
                    for h in range(2):
                        face = (k[h] + kn[h]) * (un[h] - u[h])
                        top = (k[h] + kz[h]) * (uz[h] - u[h])
                        total = (face - fl[h]) + (top - tops[x, h]) + flux_y[x, h]
                        new = u[h] + total
                        if final:
                            shots[h, step - 1, g, x - STEPS] = new
                        else:
                            if not last:
                                tops[x, h] = top
                            ud[zp, x, h] = new
                            kd[zp, x, h] = cond[z, x, h] + cond_g[z, x, h] * (new * new)
                        fr.append(face)
                    u, k, fl = un, kn, fr
                if flux is not None:
                    keep_y(flux, first, flux_y)
            if last and not final:
                for x in range(step, ext - step):
                    for h in range(2):
                        flux_y[x, h] = flux_next[x, h]

        def first_faces(i, carry):
            for j in range(2):
                x = step + i * 2 + j
                for h in range(2):
                    du = us[begin + 1, x, h] - us[begin + 1 - way, x, h]
                    tops[x, h] = (ks[begin + 1, x, h] + ks[begin + 1 - way, x, h]) * du
            return carry

        def slabs(i, carry):
            one_slab(begin + way * i, False)
            return carry

        lax.fori_loop(0, (ext - 2 * step) // 2, first_faces, 0)
        if not final:
            lax.fori_loop(0, number - 1, slabs, 0)
        one_slab(begin + way * (number - 1), True)
        if not final:

            @pl.when(strip == 0)
            def _():
                blank([(ud, 1)], 0, STEPS)

            @pl.when(strip == n_strip - 1)
            def _():
                blank([(ud, 1)], STEPS + rows_x, STEPS)

            def keep(i, carry):
                for j in range(8):
                    x = i * 8 + j
                    for h in range(2):
                        shots[h, step - 1, g, x] = ud[slab + 1, x + STEPS, h]
                return carry

            lax.fori_loop(0, rows_x // 8, keep, 0)

    def send(step, g):
        return pltpu.make_async_remote_copy(
            src_ref=shots.at[1 - core, step - 1, g],
            dst_ref=landed.at[step - 1, g],
            send_sem=send_sem.at[step - 1, g],
            recv_sem=recv_sem.at[step - 1, g],
            device_id={"run": partner},
            device_id_type=MESH,
        )

    def group(g, carry):
        @pl.when(g > 0)
        def _():
            fill(0, ext, 2, *prepare(g))

        everywhere = [(cond, 0), (cond_g, 0), (u_a, 1), (k_a, 1)]

        @pl.when(strip == 0)
        def _():
            blank(everywhere, 0, STEPS)

        @pl.when(strip == n_strip - 1)
        def _():
            blank(everywhere, STEPS + rows_x, STEPS)

        start_y(u_a, k_a)
        pairs = [(u_a, k_a), (u_b, k_b)]
        for step in range(1, STEPS + 1):
            src, dst = pairs[(step - 1) % 2], pairs[step % 2]
            advance(step, g, *src, *dst)
            send(step, g).start()
        return carry

    consts = prepare(0)
    for copy in local:
        copy.wait()
    fill(STEPS, rows_x // 2, 2, *consts)
    pl.semaphore_wait(barrier, n_run + n_strip - 2)
    for copy in halos + fetches:
        copy.start()
    fill(STEPS + rows_x // 2, rows_x // 2, 2, *consts)
    hidden_layer(vals, w_in, core, mixed, hid, hid_b, hid_t)
    hid_put.start()
    for copy in halos:
        copy.wait()
    fill(0, STEPS, 2, *consts)
    fill(STEPS + rows_x, STEPS, 2, *consts)
    lax.fori_loop(0, 2, group, 0)
    for copy in fetches:
        copy.wait()
    back[...] = jnp.zeros_like(back)
    for g in range(2):
        for step in range(1, STEPS + 1):
            send(step, g).wait()

    batch = hid.shape[0]

    def put(i):
        return pltpu.make_async_copy(e_all.at[i], error_out.at[i], e_sem.at[i])

    def train(i):
        w = jnp.swapaxes(w_all[i], 0, 1)
        w = jnp.concatenate([w[x] for x in range(WIDTH)], axis=1)
        pred = jnp.dot(hid_b[...], w, preferred_element_type=F32)
        cuts = []
        for x in range(WIDTH):
            at = i * WIDTH + x
            tiles = [shots[core, t, g, at] for t in range(STEPS) for g in range(2)]
            tiles += [landed[t, g, at] for t in range(STEPS) for g in range(2)]
            cuts.append(jnp.concatenate(tiles, axis=0))
        goal = jnp.concatenate(cuts, axis=1)
        error = ((pred - goal.astype(F32)) * (batch ** -0.5)).astype(BF)
        e_all[i] = error
        put(i).start()
        return lax.dot_general(error, w, (((1,), (1,)), ((), ())), preferred_element_type=F32)

    def several(i, carry):
        back[...] += sum(train(i * TURN + j) for j in range(TURN))
        return carry

    lax.fori_loop(0, blocks // TURN, several, 0)
    input_gradient(values, core, hid, back, partial)
    reduce_scatter(
        n_run, n_strip, partial, grad_out, got_run, mid, got_strip, s_run, r_run, s_strip, r_strip
    )
    hid_put.wait()
    for i in range(blocks):
        put(i).wait()


def hidden_layer(vals, w_in, core, mixed, hid, hid_b, hid_t):
    half = 2 * GROUP
    total = vals[:, 0:1] * w_in[0:1, :]
    for p in range(1, 6):
        total = total + vals[:, p : p + 1] * w_in[p : p + 1, :]
    mixed[...] = total
    for part in range(2):
        owner = core if part == 0 else 1 - core
        rows = mixed[pl.ds(pl.multiple_of(owner * half, half), half), :]
        for t in range(STEPS):
            pre = rows + ((t + 1.0) / STEPS) * w_in[6:7, :] + w_in[7:8, :]
            hid[pl.ds((part * STEPS + t) * half, half), :] = jnp.tanh(pre)
    hid_b[...] = hid[...].astype(BF)
    hid_t[...] = hid[...].T.astype(BF)


def input_gradient(values, core, hid, back, partial):
    half = 2 * GROUP
    h = hid[...]
    slope = back[...] * (1.0 - h * h)
    steps = [
        [slope[(part * STEPS + t) * half : (part * STEPS + t + 1) * half] for t in range(STEPS)]
        for part in range(2)
    ]
    runs = [p[0] + p[1] + p[2] + p[3] for p in steps]
    vals = [
        values[pl.ds(pl.multiple_of((core if part == 0 else 1 - core) * half, half), half), :]
        for part in range(2)
    ]
    rows = []
    for p in range(6):
        both = vals[0][:, p : p + 1] * runs[0] + vals[1][:, p : p + 1] * runs[1]
        rows.append(jnp.sum(both, axis=0, keepdims=True))
    timed = sum(((t + 1.0) / STEPS) * (steps[0][t] + steps[1][t]) for t in range(STEPS))
    rows.append(jnp.sum(timed, axis=0, keepdims=True))
    rows.append(jnp.sum(runs[0] + runs[1], axis=0, keepdims=True))
    full = jnp.concatenate(rows, axis=0)
    for q in range(partial.shape[0]):
        partial[q] = full[:, q * LANES : (q + 1) * LANES]


def reduce_scatter(
    n_run, n_strip, partial, out, got_run, mid, got_strip, s_run, r_run, s_strip, r_strip
):
    run = lax.axis_index("run")
    strip = lax.axis_index("strip")
    units = partial.shape[0] * LANES
    keep = units // (n_run * n_strip)
    per = LANES // (n_strip * keep)
    copies = []
    for j in range(1, n_run):
        to = lax.rem(run + j, n_run)
        copies.append(
            pltpu.make_async_remote_copy(
                src_ref=partial.at[lax.div(to, per)],
                dst_ref=got_run.at[j - 1],
                send_sem=s_run.at[j - 1],
                recv_sem=r_run.at[j - 1],
                device_id={"run": to},
                device_id_type=MESH,
            )
        )
        copies[-1].start()
    total = partial[lax.div(run, per)]
    for j in range(n_run - 1):
        copies[j].wait_recv()
        total = total + got_run[j]
    mid[...] = total
    more = []
    for j in range(1, n_strip):
        to = lax.rem(strip + j, n_strip)
        more.append(
            pltpu.make_async_remote_copy(
                src_ref=mid,
                dst_ref=got_strip.at[j - 1],
                send_sem=s_strip.at[j - 1],
                recv_sem=r_strip.at[j - 1],
                device_id={"strip": to},
                device_id_type=MESH,
            )
        )
        more[-1].start()
    for j in range(n_strip - 1):
        more[j].wait_recv()
        total = total + got_strip[j]
    for copy in copies + more:
        copy.wait_send()
    at = lax.rem(run, per) * (n_strip * keep) + strip * keep
    out[...] = pltpu.roll(total, lax.rem(LANES - at, LANES), 1)


def forward(levels, index, w_in, base, material, weight, n_run, n_strip):
    rows_x, nz, ny = base.shape
    units = weight.shape[0]
    batch = STEPS * index.shape[1]
    blocks = rows_x // WIDTH
    ext = rows_x + 2 * STEPS
    hbm = pl.BlockSpec(memory_space=pl.ANY)
    vmem = pl.BlockSpec(memory_space=pltpu.VMEM)
    dma = pltpu.SemaphoreType.DMA
    return pl.pallas_call(
        functools.partial(forward_kernel, n_run, n_strip),
        out_shape=(
            jax.ShapeDtypeStruct((blocks, batch, WIDTH * LANES), BF),
            jax.ShapeDtypeStruct((units, batch), BF),
            jax.ShapeDtypeStruct((8, LANES), F32),
        ),
        in_specs=[hbm] * 6,
        out_specs=(hbm, hbm, vmem),
        scratch_shapes=[
            pltpu.VMEM((ext, nz, ny), F32),
            pltpu.VMEM((ext, nz, ny), jnp.int32),
            pltpu.VMEM((2, STEPS, 2, rows_x, GROUP, LANES), BF),
            pltpu.VMEM((STEPS, 2, rows_x, GROUP, LANES), BF),
            pltpu.VMEM((index.shape[1], 8), F32),
            pltpu.VMEM((units // LANES, 8, LANES), F32),
            pltpu.VMEM((n_run - 1, 8, LANES), F32),
            pltpu.VMEM((8, LANES), F32),
            pltpu.VMEM((n_strip - 1, 8, LANES), F32),
            dma((2,)), dma((4,)), dma((4,)), dma((4,)), dma((STEPS, 2)), dma((STEPS, 2)),
            dma((blocks,)), dma((blocks,)),
            dma((n_run - 1,)), dma((n_run - 1,)), dma((n_strip - 1,)), dma((n_strip - 1,)),
        ],
        compiler_params=pltpu.CompilerParams(
            collective_id=0, has_side_effects=True, vmem_limit_bytes=63 * 1024 * 1024
        ),
        name="forward",
    )(levels, index, w_in, base, material, weight)


def output_kernel(
    hid_in, total_in, error, grad, turned, hid, total, e_all, g_all, h_sem, t_sem, e_sem, g_sem
):
    blocks = e_all.shape[0]
    fetches = [pltpu.make_async_copy(error.at[i], e_all.at[i], e_sem.at[i]) for i in range(blocks)]
    first = pltpu.make_async_copy(hid_in, hid, h_sem)
    second = pltpu.make_async_copy(total_in, total, t_sem)
    for copy in [first, *fetches[:AHEAD], second]:
        copy.start()
    puts = []
    first.wait()
    for i in range(blocks):
        fetches[i].wait()
        if i + AHEAD < blocks:
            fetches[i + AHEAD].start()
        g = jnp.dot(hid[...], e_all[i], preferred_element_type=F32).astype(BF)
        g = jnp.stack([g[:, x * LANES : (x + 1) * LANES] for x in range(WIDTH)], axis=0)
        g_all[i] = jnp.swapaxes(g, 0, 1)
        puts.append(
            pltpu.make_async_copy(
                g_all.at[i], grad.at[:, pl.ds(i * WIDTH, WIDTH), :], g_sem.at[i]
            )
        )
        puts[-1].start()
    second.wait()
    turned[...] = total[...].T[: turned.shape[0]]
    for copy in puts:
        copy.wait()


def output_gradient(hid, total, error, keep):
    units, batch = hid.shape
    blocks = error.shape[0]
    hbm = pl.BlockSpec(memory_space=pl.ANY)
    vmem = pl.BlockSpec(memory_space=pltpu.VMEM)
    return pl.pallas_call(
        output_kernel,
        out_shape=(
            jax.ShapeDtypeStruct((units, blocks * WIDTH, LANES), BF),
            jax.ShapeDtypeStruct((keep, 8), F32),
        ),
        in_specs=[hbm, hbm, hbm],
        out_specs=(hbm, vmem),
        scratch_shapes=[
            pltpu.VMEM(hid.shape, BF),
            pltpu.VMEM(total.shape, F32),
            pltpu.VMEM(error.shape, BF),
            pltpu.VMEM((blocks, units, WIDTH, LANES), BF),
            pltpu.SemaphoreType.DMA,
            pltpu.SemaphoreType.DMA,
            pltpu.SemaphoreType.DMA((blocks,)),
            pltpu.SemaphoreType.DMA((blocks,)),
        ],
        compiler_params=pltpu.CompilerParams(vmem_limit_bytes=63 * 1024 * 1024),
        name="output_gradient",
    )(hid, total, error)


def solution(mesh):
    n_run, n_strip = mesh.shape["run"], mesh.shape["strip"]

    def local(base_field, material_map, param_levels, param_index, w_input, w_output):
        error, hid, total = forward(
            param_levels, param_index.T, w_input, base_field, material_map, w_output, n_run, n_strip
        )
        keep = w_output.shape[0] // (n_run * n_strip)
        grad_output, turned = output_gradient(hid, total, error, keep)
        return grad_output, turned.T

    placed = (
        P("strip", None, None),
        P("strip", None, None),
        P(),
        P(),
        P(),
        P(None, "strip", "run"),
    )
    return jax.shard_map(
        local,
        mesh=mesh,
        in_specs=placed,
        out_specs=(P(None, "strip", "run"), P(None, ("run", "strip"))),
        check_vma=False,
    )
```
